32 devices in a mesh: req: 8 (over y, x, core), head: 4 (over z).
Axes of the slice: x: 2, y: 2, z: 4, core: 2. Of those that a mesh axis runs over, the one named last changes fastest.
Arguments:
- queries: bfloat16 [128, 64, 128], P('req', 'head'), may hold values from -6 to 6
- k_codes: bfloat16 [8192, 16, 8, 128], P('req', None, 'head'), may hold values from -6 to 6
- value_quantized_codes: bfloat16 [8192, 16, 8, 128], P('req', None, 'head'), may hold values from -6 to 6
- key_page_scale: float32 [8192, 8], P('req', 'head'), may hold values from 0.5 to 2
- value_page_scale: float32 [8192, 8], P('req', 'head'), may hold values from 4 to 16
- lengths: int32 [128], P('req'), may hold values from 1 to 2032
- page_table: int32 [128, 128], P('req'), may hold values from -1 to 8191, as said below
- out_weight: bfloat16 [8192, 8192], P('head', 'req'), may hold values from -0.0625 to 0.0625
Outputs:
- attn_out: bfloat16 [128, 8192], P(None, ('req', 'head'))
The draws below stay inside these ranges and needn't reach their ends.
Inputs may be any that keep to these rules, and one draw needn't show every extreme that they name: `page_table`: entries j below ceil(lengths[r] / 16) name pool pages; all such entries of all requests together name every pool page exactly once. Entries beyond are -1.
All inputs are finite; a program needn't handle non-finite values.
Results may differ from the reference program's by a relative error of at most 0.02.
Values may be sent and summed in bfloat16 or wider, within the bound.
A program may use at most 128 MiB of HBM per device.

```python
import math
import jax
import jax.numpy as jnp
from jax import lax

QUERY_HEADS = 64
KEY_VALUE_HEADS = 8
HEAD_DIMENSION = 128
DMODEL = 8192
PAGE_TOKENS = 16
MAXP = 128
R_DEV = 16
REQS = 128
POOL_PAGES = 8192
N_REQ = 8


def page_layout(key):
    half_count = REQS // 2
    middle = MAXP // 2
    sign_dev = 2 * jax.random.randint(jax.random.fold_in(key, 1), (N_REQ // 2,), 0, 2) - 1
    shift = jax.random.randint(jax.random.fold_in(key, 2), (half_count,), 0, middle)
    selected_pages = jax.random.randint(jax.random.fold_in(key, 3), (), 0, half_count)
    shift = shift.at[selected_pages].set(middle - 1)
    owner_dev = jnp.arange(half_count, dtype=jnp.int32) // R_DEV
    turned = sign_dev[owner_dev] * shift
    page_count = jnp.concatenate([middle + turned, middle - turned]).astype(jnp.int32)
    remainder = jax.random.randint(jax.random.fold_in(key, 4), (REQS,), 1, PAGE_TOKENS + 1)
    longest = jnp.where(sign_dev[selected_pages // R_DEV] > 0, selected_pages, selected_pages + half_count)
    remainder = remainder.at[longest].set(PAGE_TOKENS)
    lengths = ((page_count - 1) * PAGE_TOKENS + remainder).astype(jnp.int32)
    shuffled = jax.random.permutation(jax.random.fold_in(key, 5), POOL_PAGES).astype(jnp.int32)
    starts = jnp.cumsum(page_count) - page_count
    entry = jnp.arange(MAXP, dtype=jnp.int32)[None, :]
    slot = jnp.clip(starts[:, None] + entry, 0, POOL_PAGES - 1)
    table = jnp.where(entry < page_count[:, None], shuffled[slot], -1).astype(jnp.int32)
    return (lengths, table)


def draw_lengths(key, part):
    return page_layout(jax.random.fold_in(key, 11))[0]


def draw_page_table(key, part):
    return page_layout(jax.random.fold_in(key, 11))[1]


def draw_queries(key, part):
    value_rows = jnp.clip(jax.random.normal(jax.random.fold_in(key, 21), (REQS, QUERY_HEADS, HEAD_DIMENSION), jnp.float32), -6.0, 6.0)
    return value_rows.astype(jnp.bfloat16)


def draw_k_codes(key, part):
    value_rows = jnp.clip(jax.random.normal(jax.random.fold_in(key, 31), (POOL_PAGES, PAGE_TOKENS, KEY_VALUE_HEADS, HEAD_DIMENSION), jnp.float32), -6.0, 6.0)
    return value_rows.astype(jnp.bfloat16)


def steps_of(rng, extent, split, smallest, high):
    level = 1.0
    for dim, parts in split:
        draws = jax.random.uniform(jax.random.fold_in(jax.random.fold_in(rng, 6), dim), (parts,), jnp.float32, smallest / len(split), high / len(split))
        level = level * jnp.repeat(jnp.exp(draws), extent[dim] // parts).reshape((-1,) + (1,) * (len(extent) - 1 - dim))
    return level


def normal_values(key, extent, width, reach, shards=(), held_as=jnp.bfloat16):
    level = steps_of(key, extent, shards, -0.22, 0.18) if shards else 1.0
    array = jax.random.normal(key, extent, jnp.float32) * width * level
    return jnp.minimum(jnp.maximum(array, -reach), reach).astype(held_as)


def setup_inputs(seed: int = 0) -> dict:
    arg_keys = jax.random.split(jax.random.key(seed), 9)
    queries = draw_queries(jax.random.fold_in(arg_keys[8], 71), 0)
    k_codes = draw_k_codes(jax.random.fold_in(arg_keys[8], 71), 0)
    value_quantized_codes = normal_values(arg_keys[2], (POOL_PAGES, PAGE_TOKENS, KEY_VALUE_HEADS, HEAD_DIMENSION), 1.0, 6.0, ((0, 8), (2, 4)))
    key_page_scale = jnp.clip(jnp.exp(math.log(2.0) - 1.3862944 * jax.random.uniform(arg_keys[3], (POOL_PAGES, KEY_VALUE_HEADS), jnp.float32) ** steps_of(arg_keys[3], (POOL_PAGES, KEY_VALUE_HEADS), ((0, 8), (1, 4)), -0.2, 0.2)), 0.5, 2.0)
    value_page_scale = jnp.clip(jnp.exp(math.log(16.0) - 1.3862944 * jax.random.uniform(arg_keys[4], (POOL_PAGES, KEY_VALUE_HEADS), jnp.float32) ** steps_of(arg_keys[4], (POOL_PAGES, KEY_VALUE_HEADS), ((0, 8), (1, 4)), -0.2, 0.2)), 4.0, 16.0)
    lengths = draw_lengths(jax.random.fold_in(arg_keys[8], 71), 0)
    page_table = draw_page_table(jax.random.fold_in(arg_keys[8], 71), 0)
    out_weight = normal_values(arg_keys[7], (QUERY_HEADS * HEAD_DIMENSION, DMODEL), (QUERY_HEADS * HEAD_DIMENSION) ** -0.5, 0.0625, ((0, 4), (1, 8)))
    return {"queries": queries, "k_codes": k_codes, "value_quantized_codes": value_quantized_codes, "key_page_scale": key_page_scale, "value_page_scale": value_page_scale, "lengths": lengths, "page_table": page_table, "out_weight": out_weight}


floor_score = -1e+30

def reference(queries, k_codes, value_quantized_codes, key_page_scale, value_page_scale, lengths, page_table, out_weight):
    query_group_count = QUERY_HEADS // KEY_VALUE_HEADS

    def per_request(inputs_row):
        query_vector, length_row, table_row = inputs_row
        page_ids = jnp.maximum(table_row, 0).astype(jnp.int32)
        keys = k_codes[page_ids].astype(jnp.float32)
        value_rows = value_quantized_codes[page_ids].astype(jnp.float32)
        query_float = query_vector.astype(jnp.float32).reshape(KEY_VALUE_HEADS, query_group_count, HEAD_DIMENSION)
        scores = jnp.einsum('kgd,ptkd->pkgt', query_float, keys)
        scores = scores * (key_page_scale[page_ids][:, :, None, None] / math.sqrt(HEAD_DIMENSION))
        position = jnp.arange(MAXP, dtype=jnp.int32)[:, None] * PAGE_TOKENS + jnp.arange(PAGE_TOKENS, dtype=jnp.int32)[None, :]
        is_live = (position < length_row)[:, None, None, :]
        page_max = lax.optimization_barrier(jnp.max(jnp.where(is_live, scores, floor_score), axis=-1))
        weights = jnp.where(is_live, jnp.exp(scores - page_max[..., None]), 0.0)
        weights = lax.optimization_barrier(weights.astype(jnp.bfloat16)).astype(jnp.float32)
        page_sum = lax.optimization_barrier(jnp.sum(weights, axis=-1))
        page_out = jnp.einsum('pkgt,ptkd->pkgd', weights, value_rows) * value_page_scale[page_ids][:, :, None, None]
        peak = lax.optimization_barrier(jnp.max(page_max, axis=0))
        factor = jnp.exp(page_max - peak)
        numerator = lax.optimization_barrier(jnp.sum(page_out * factor[..., None], axis=0))
        denominator = lax.optimization_barrier(jnp.sum(page_sum * factor, axis=0))
        return (numerator / denominator[..., None]).reshape(QUERY_HEADS * HEAD_DIMENSION)
    attention = lax.map(per_request, (queries, lengths, page_table))
    return jnp.dot(attention.astype(jnp.bfloat16), out_weight, preferred_element_type=jnp.float32).astype(jnp.bfloat16)
```

```python
import functools
import math

import jax
import jax.numpy as jnp
from jax import lax
from jax.experimental import pallas as pl
from jax.experimental.pallas import tpu as pltpu
from jax.sharding import PartitionSpec as P

MESH = pl.DeviceIdType.MESH
FLOOR = -1e30
DROP = -3e38
LANES = 128
SUB = 8
LIVE_BITS = 5
ROUND = 8
F32 = jnp.float32
BF16 = jnp.bfloat16
I32 = jnp.int32


def nt(a, b):
    return lax.dot_general(a, b, (((1,), (1,)), ((), ())), preferred_element_type=F32)


def nn(a, b):
    return jnp.dot(a, b, preferred_element_type=F32)


def iota(shape, axis):
    return lax.broadcasted_iota(I32, shape, axis)


def list_kernel(cfg, lengths_ref, table_ref, out_ref):
    sources, rows_here, pages = cfg["sources"], cfg["rows_here"], cfg["pages"]
    page_size, per_group = cfg["page_size"], cfg["per_group"]
    slot_rows, group_rows = cfg["slot_rows"], cfg["group_rows"]
    shape = (rows_here, LANES)
    row_id = iota(shape, 0)
    lengths = jnp.zeros(shape, I32)
    for r in range(rows_here):
        lengths = jnp.where(row_id == r, lengths_ref[r], lengths)
    live = jnp.minimum(lengths - iota(shape, 1) * page_size, page_size)
    table = table_ref[...]
    locals_, mines = [], []
    for d in range(sources):
        local = table - d * pages
        locals_.append(local)
        mines.append((live > 0) & (local >= 0) & (local < pages))
    flag = jnp.concatenate([jnp.where(m, 1.0, 0.0) for m in mines], axis=0).astype(BF16)
    total = sources * rows_here
    up = jnp.where(iota((LANES, LANES), 0) < iota((LANES, LANES), 1), 1.0, 0.0).astype(BF16)
    before = nn(flag, up)
    count = nn(flag, jnp.ones((LANES, LANES), BF16))
    need = jnp.floor((count + (per_group - 1)) * (1.0 / per_group))
    i, j = iota((total, total), 0), iota((total, total), 1)
    tri = jnp.where((i >= j) & (i // rows_here == j // rows_here), 1.0, 0.0).astype(BF16)
    ends = nn(tri, need.astype(BF16))
    starts = ends - need
    slots = (starts * per_group + before).astype(I32)

    key = jnp.full(shape, -1, I32)
    page = jnp.zeros(shape, I32)
    for d in range(sources):
        slot = slots[d * rows_here : (d + 1) * rows_here] + d * (slot_rows * LANES)
        key = jnp.where(mines[d], slot, key)
        page = jnp.where(mines[d], locals_[d], page)
    one = (page >> 2).astype(F32)
    two = ((page & 3) * (1 << LIVE_BITS) + live).astype(F32)
    high, low = key >> 7, key & (LANES - 1)
    hi_rows = -(-(sources * slot_rows) // 16) * 16
    hi_iota, lo_iota = iota((hi_rows, LANES), 0), iota((LANES, LANES), 0)
    lefts, rights = [], []
    for r in range(rows_here):
        row = slice(r, r + 1)
        lefts.append(jnp.where(hi_iota == high[row], 1.0, 0.0).astype(BF16))
        same = lo_iota == low[row]
        pair = [jnp.where(same, one[row], 0.0), jnp.where(same, two[row], 0.0)]
        rights.append(jnp.concatenate(pair, axis=0).astype(BF16))
    found = nt(jnp.concatenate(lefts, axis=1), jnp.concatenate(rights, axis=1))
    found = (found[:, :LANES] * float(4 << LIVE_BITS) + found[:, LANES:]).astype(I32)

    lane = iota(shape, 1).astype(F32)
    diag = row_id == iota(shape, 1)
    for d in range(sources):
        rows = slice(d * rows_here, (d + 1) * rows_here)
        end, begin, some = ends[rows], starts[rows], need[rows] > 0.5
        out_ref[d, :slot_rows, :] = found[d * slot_rows : (d + 1) * slot_rows]
        for b in range(group_rows):
            here = lane + float(b * LANES)
            done = end <= here
            owner = jnp.sum(jnp.where(done, 1.0, 0.0), axis=0, keepdims=True)
            owner = jnp.minimum(owner, float(rows_here - 1))
            last = jnp.min(jnp.where(done, 4096.0, end), axis=0, keepdims=True) - 1.0
            opens = jnp.where((begin == here) & some, 1.0, 0.0)
            opens = jnp.max(opens, axis=0, keepdims=True)
            value = (last * 2.0 + (1.0 - opens)) * float(rows_here) + owner
            out_ref[d, slot_rows + b : slot_rows + b + 1, :] = value.astype(I32)
        mark = jnp.maximum(end - 1.0, 0.0) * 2.0 + jnp.where(some, 1.0, 0.0)
        mark = jnp.sum(jnp.where(diag, mark, 0.0), axis=0, keepdims=True)
        size = jnp.maximum(jnp.max(end, axis=0, keepdims=True), 1.0)
        mark = jnp.where(iota((1, LANES), 1) == rows_here, size, mark)
        base = slot_rows + group_rows
        out_ref[d, base : base + 1, :] = mark.astype(I32)


def kernel(
    cfg,
    info_ref,
    kscale_ref,
    vscale_ref,
    q_hbm,
    k_hbm,
    v_hbm,
    w_hbm,
    out_ref,
    info_all,
    info,
    q_all,
    k_buf,
    v_buf,
    w_buf,
    kse,
    vse,
    scores,
    peaks,
    dens,
    accs,
    num_send,
    lse_send,
    num_recv,
    lse_recv,
    mixed,
    att_all,
    term_send,
    term_recv,
    q_sem,
    load_sems,
    info_sem,
    smem_sem,
    t_send,
    t_recv,
    q_send,
    q_recv,
    n_send,
    n_recv,
    l_send,
    l_recv,
    a_send,
    a_recv,
    z_send,
    z_recv,
):
    sources, nz = cfg["sources"], cfg["nz"]
    rows_here, heads, dim = cfg["rows_here"], cfg["heads"], cfg["dim"]
    pages, page_rows, page_size = cfg["pages"], cfg["page_rows"], cfg["page_size"]
    requests = rows_here * sources
    kv_local = page_rows // page_size
    per_group = LANES // page_rows
    n_groups = cfg["n_groups"]
    steps = n_groups // ROUND
    width = heads * dim
    me = lax.axis_index("req")
    mz = lax.axis_index("head")
    slot_rows, mark_row = cfg["slot_rows"], cfg["slot_rows"] + cfg["group_rows"]

    q_load = pltpu.make_async_copy(q_hbm, q_all.at[pl.ds(me * rows_here, rows_here)], q_sem)
    q_load.start()
    info_load = pltpu.make_async_copy(info_ref.at[me], info_all.at[me], info_sem)
    info_load.start()
    loads = []
    parts = load_sems.shape[1]
    for which, (src, dst) in enumerate(((k_hbm, k_buf), (v_hbm, v_buf), (w_hbm, w_buf))):
        chunk = src.shape[0] // parts
        for c in range(parts):
            rows = pl.ds(c * chunk, chunk)
            cp = pltpu.make_async_copy(src.at[rows], dst.at[rows], load_sems.at[which, c])
            cp.start()
            loads.append(cp)
    k_loads, v_loads, w_loads = loads[:parts], loads[parts : 2 * parts], loads[2 * parts :]

    barrier = pltpu.get_barrier_semaphore()
    for k in range(1, sources):
        pl.semaphore_signal(
            barrier, inc=1, device_id={"req": lax.rem(me + k, sources)}, device_id_type=MESH
        )
    for k in range(1, nz):
        pl.semaphore_signal(barrier, inc=1, device_id={"head": lax.rem(mz + k, nz)}, device_id_type=MESH)
    pl.semaphore_wait(barrier, sources + nz - 2)

    def info_copy(peer, owner):
        return pltpu.make_async_remote_copy(
            src_ref=info_ref.at[peer],
            dst_ref=info_all.at[owner],
            send_sem=t_send.at[peer],
            recv_sem=t_recv.at[owner],
            device_id={"req": peer},
            device_id_type=MESH,
        )

    def q_copy(k, owner):
        peer = lax.rem(me + k, sources)
        rows = pl.ds(owner * rows_here, rows_here)
        return pltpu.make_async_remote_copy(
            src_ref=q_all.at[rows],
            dst_ref=q_all.at[rows],
            send_sem=q_send.at[peer],
            recv_sem=q_recv.at[owner],
            device_id={"req": peer},
            device_id_type=MESH,
        )

    for k in range(1, sources):
        info_copy(lax.rem(me + k, sources), me).start()
    q_load.wait()
    for k in range(1, sources):
        q_copy(k, me).start()

    lane_sub = iota((LANES, LANES), 0)
    for src, dst, factor in ((kscale_ref, kse, 1.0 / math.sqrt(dim)), (vscale_ref, vse, 1.0)):
        for b in range(pages // LANES):
            cols = slice(b * LANES, (b + 1) * LANES)
            both = src[kv_local - 1 : kv_local, cols]
            for v in range(kv_local - 1):
                both = jnp.where(lane_sub % kv_local == v, src[v : v + 1, cols], both)
            both = jnp.broadcast_to(both * factor, (LANES, LANES)).T
            dst[b * LANES : (b + 1) * LANES, 0, :] = both

    info_load.wait()
    for k in range(1, sources):
        peer = lax.rem(me + k, sources)
        info_copy(peer, peer).wait_recv()
    to_smem = pltpu.make_async_copy(info_all, info, smem_sem)
    to_smem.start()
    to_smem.wait()
    for k in range(1, sources):
        q_copy(k, lax.rem(me + k, sources)).wait_recv()
    for cp in k_loads:
        cp.wait()

    lane8 = iota((SUB, LANES), 1)
    token = (lane8 % page_rows) // kv_local
    per_head = heads // kv_local
    kv_masks = [lane8 % kv_local == (t * SUB) // per_head for t in range(heads // SUB)]
    blank = jnp.zeros((heads, dim), BF16)

    def by_page(parts):
        got = parts[per_group - 1]
        for i in range(per_group - 2, -1, -1):
            got = jnp.where(lane8 < (i + 1) * page_rows, parts[i], got)
        return got

    def page_of(at, i):
        src, k = at
        lane_at = (k & (LANES // per_group - 1)) * per_group
        value = info[src, k // (LANES // per_group), lane_at + i]
        return value >> LIVE_BITS, value & ((1 << LIVE_BITS) - 1)

    def group_of(at):
        src, k = at
        value = info[src, slot_rows + k // LANES, k & (LANES - 1)]
        owner = src * rows_here + (value & (rows_here - 1))
        rest = value // rows_here
        return owner, (rest & 1).astype(F32), rest // 2

    def advance(at):
        src, k = at
        more = k + 1 < info[src, mark_row, rows_here]
        stay = more | (src + 1 >= sources)
        next_k = jnp.where(more, k + 1, jnp.where(stay, k, 0))
        return jnp.where(stay, src, src + 1), next_k

    def fetch(ref, page_ids):
        return jnp.concatenate([ref[p] for p in page_ids], axis=0)

    def scale_row(ref, page_ids):
        return by_page([jnp.broadcast_to(ref[p], (SUB, LANES)) for p in page_ids])

    def score_step(it, carry):
        top, at = carry
        for pair in range(ROUND // 2):
            ats = [at, advance(at)]
            at = advance(ats[1])
            info_of = [[page_of(one, i) for i in range(per_group)] for one in ats]
            ids = [[p for p, _ in one] for one in info_of]
            heads_of = [group_of(one) for one in ats]
            kk = jnp.concatenate([fetch(k_buf, one) for one in ids], axis=1)
            qa, qb = [q_all[owner] for owner, _, _ in heads_of]
            lhs = jnp.concatenate(
                [jnp.concatenate([qa, blank], axis=1), jnp.concatenate([blank, qb], axis=1)], axis=0
            )
            s = nt(lhs, kk)
            for x in range(2):
                g = it * ROUND + 2 * pair + x
                live_row = by_page([jnp.full((SUB, LANES), n, I32) for _, n in info_of[x]])
                is_live = token < live_row
                scale = scale_row(kse, ids[x])
                tiles = []
                for t in range(heads // SUB):
                    tile = s[x * heads + t * SUB : x * heads + (t + 1) * SUB] * scale
                    tiles.append(jnp.where(is_live & kv_masks[t], tile, FLOOR))
                tile = jnp.concatenate(tiles, axis=0)
                scores[g] = tile
                mine = jnp.broadcast_to(jnp.max(tile, axis=1, keepdims=True), (heads, LANES))
                top = jnp.maximum(top + (1.0 - heads_of[x][1]) * DROP, mine)
                peaks[g] = top
        return top, at

    first = (jnp.int32(0), jnp.int32(0))
    lax.fori_loop(0, steps, score_step, (jnp.full((heads, LANES), FLOOR, F32), first))
    for cp in v_loads:
        cp.wait()

    def value_step(it, carry):
        acc, den, at = carry
        for pair in range(ROUND // 2):
            ats = [at, advance(at)]
            at = advance(ats[1])
            ids = [[page_of(one, i)[0] for i in range(per_group)] for one in ats]
            heads_of = [group_of(one) for one in ats]
            vv = jnp.concatenate([fetch(v_buf, one) for one in ids], axis=1)
            lhs, weights = [], []
            for x in range(2):
                g = it * ROUND + 2 * pair + x
                last = g - ats[x][1] + heads_of[x][2]
                weight = jnp.exp(scores[g] - peaks[last])
                scale = scale_row(vse, ids[x])
                scaled = [weight[t * SUB : (t + 1) * SUB] * scale for t in range(heads // SUB)]
                lhs.append(jnp.concatenate(scaled, axis=0).astype(BF16))
                weights.append(weight)
            o = nn(jnp.concatenate(lhs, axis=0), vv)
            for x in range(2):
                g = it * ROUND + 2 * pair + x
                keep = heads_of[x][1]
                acc = acc * keep + o[x * heads : (x + 1) * heads, x * dim : (x + 1) * dim]
                den = den * keep + weights[x]
                accs[g] = acc
                dens[g] = den
        return acc, den, at

    zero = jnp.zeros((heads, LANES), F32)
    lax.fori_loop(0, steps, value_step, (zero, zero, first))

    lane16 = iota((heads, LANES), 1)

    def outgoing(dest, num_at, lse_at):
        lse_tile = jnp.full((heads, LANES), FLOOR, F32)
        base = jnp.int32(0)
        for src in range(sources):
            base = base + jnp.where(src < dest, info[src, mark_row, rows_here], 0)
        for r in range(rows_here):
            mark = info[dest, mark_row, r]
            last = base + mark // 2
            some = (mark & 1).astype(F32)
            den = jnp.broadcast_to(jnp.sum(dens[last], axis=1, keepdims=True), (heads, LANES))
            den = jnp.maximum(den, 0.5)
            num_at[r] = (accs[last] * (some / den)).astype(BF16)
            lse = (peaks[last] + jnp.log(den)) * some + (some - 1.0) * (-FLOOR)
            lse_tile = jnp.where(lane16 == r, lse, lse_tile)
        lse_at[...] = lse_tile

    def num_copy(peer, owner):
        return pltpu.make_async_remote_copy(
            src_ref=num_send.at[peer],
            dst_ref=num_recv.at[owner],
            send_sem=n_send.at[peer],
            recv_sem=n_recv.at[owner],
            device_id={"req": peer},
            device_id_type=MESH,
        )

    def lse_copy(peer, owner):
        return pltpu.make_async_remote_copy(
            src_ref=lse_send.at[peer],
            dst_ref=lse_recv.at[owner],
            send_sem=l_send.at[peer],
            recv_sem=l_recv.at[owner],
            device_id={"req": peer},
            device_id_type=MESH,
        )

    def send_block(k, carry):
        peer = lax.rem(me + k, sources)
        outgoing(peer, num_send.at[peer], lse_send.at[peer])
        num_copy(peer, me).start()
        lse_copy(peer, me).start()
        return carry

    lax.fori_loop(1, sources, send_block, 0)
    outgoing(me, num_recv.at[me], lse_recv.at[me])
    for k in range(1, sources):
        peer = lax.rem(me + k, sources)
        lse_copy(peer, peer).wait_recv()
    for k in range(1, sources):
        peer = lax.rem(me + k, sources)
        num_copy(peer, peer).wait_recv()

    lses = [lse_recv[s] for s in range(sources)]
    top = functools.reduce(jnp.maximum, lses)
    shares = [jnp.exp(x - top) for x in lses]
    total = functools.reduce(jnp.add, shares)
    shares = [x / total for x in shares]
    for r in range(rows_here):
        got = jnp.zeros((heads, dim), F32)
        for s in range(sources):
            share = jnp.broadcast_to(shares[s][:, r : r + 1], (heads, dim))
            got = got + share * num_recv[s, r].astype(F32)
        mixed[r * heads : (r + 1) * heads, :] = got
    for h in range(heads):
        rows = mixed[pl.ds(h, rows_here, stride=heads), :]
        att_all[me, :, h * dim : (h + 1) * dim] = rows.astype(BF16)

    def att_copy(peer, owner):
        return pltpu.make_async_remote_copy(
            src_ref=att_all.at[owner],
            dst_ref=att_all.at[owner],
            send_sem=a_send.at[peer],
            recv_sem=a_recv.at[owner],
            device_id={"req": peer},
            device_id_type=MESH,
        )

    for k in range(1, sources):
        att_copy(lax.rem(me + k, sources), me).start()
    for cp in w_loads:
        cp.wait()
    for k in range(1, sources):
        peer = lax.rem(me + k, sources)
        att_copy(peer, peer).wait_recv()

    att = att_all[...].reshape(requests, width)
    cols = w_buf.shape[1] // nz

    def term_copy(peer, owner):
        return pltpu.make_async_remote_copy(
            src_ref=term_send.at[peer],
            dst_ref=term_recv.at[owner],
            send_sem=z_send.at[peer],
            recv_sem=z_recv.at[owner],
            device_id={"head": peer},
            device_id_type=MESH,
        )

    def project(z):
        return nn(att, w_buf[:, pl.ds(pl.multiple_of(z * cols, cols), cols)])

    if cols % LANES == 0:
        for k in range(1, nz):
            peer = lax.rem(mz + k, nz)
            term_send[peer] = project(peer).astype(BF16)
            term_copy(peer, mz).start()
        result = project(mz)
    else:
        every = nn(att, w_buf[...])
        for z in range(nz):
            term_send[z] = every[:, z * cols : (z + 1) * cols].astype(BF16)
        for k in range(1, nz):
            term_copy(lax.rem(mz + k, nz), mz).start()
        result = term_send[mz].astype(F32)
    for k in range(1, nz):
        peer = lax.rem(mz + k, nz)
        term_copy(peer, peer).wait_recv()
        result = result + term_recv[peer].astype(F32)
    out_ref[...] = result.astype(BF16)

    for k in range(1, sources):
        peer = lax.rem(me + k, sources)
        info_copy(peer, me).wait_send()
        q_copy(k, me).wait_send()
        num_copy(peer, me).wait_send()
        lse_copy(peer, me).wait_send()
        att_copy(peer, me).wait_send()
    for k in range(1, nz):
        term_copy(lax.rem(mz + k, nz), mz).wait_send()


def on_device(
    queries,
    k_codes,
    value_quantized_codes,
    key_page_scale,
    value_page_scale,
    lengths,
    page_table,
    out_weight,
):
    pages, page_size, kv_local, dim = k_codes.shape
    rows_here, heads, _ = queries.shape
    sources, nz = lax.axis_size("req"), lax.axis_size("head")
    requests = rows_here * sources
    page_rows = page_size * kv_local
    per_group = LANES // page_rows
    group_bound = (pages + (per_group - 1) * requests) // per_group + sources
    n_groups = -(-group_bound // ROUND) * ROUND
    list_bound = (pages + (per_group - 1) * rows_here) // per_group
    slot_rows = -(-list_bound * per_group // LANES)
    group_rows = -(-list_bound // LANES)
    info_rows = -(-(slot_rows + group_rows + 1) // SUB) * SUB
    k_rows = k_codes.reshape(pages, page_rows, dim)
    v_rows = value_quantized_codes.reshape(pages, page_rows, dim)
    width = heads * dim
    columns = out_weight.shape[1]
    cfg = dict(
        sources=sources,
        nz=nz,
        rows_here=rows_here,
        heads=heads,
        dim=dim,
        pages=pages,
        page_rows=page_rows,
        page_size=page_size,
        n_groups=n_groups,
        per_group=per_group,
        slot_rows=slot_rows,
        group_rows=group_rows,
    )
    vmem = pl.BlockSpec(memory_space=pltpu.VMEM)
    smem = pl.BlockSpec(memory_space=pltpu.SMEM)
    hbm = pl.BlockSpec(memory_space=pl.ANY)
    dma = pltpu.SemaphoreType.DMA
    info = pl.pallas_call(
        functools.partial(list_kernel, cfg),
        out_shape=jax.ShapeDtypeStruct((sources, info_rows, LANES), I32),
        in_specs=[smem, vmem],
        out_specs=vmem,
        name="lists",
    )(lengths, page_table)
    return pl.pallas_call(
        functools.partial(kernel, cfg),
        out_shape=jax.ShapeDtypeStruct((requests, columns // nz), BF16),
        in_specs=[vmem, vmem, vmem, hbm, hbm, hbm, hbm],
        out_specs=vmem,
        scratch_shapes=[
            pltpu.VMEM(info.shape, I32),
            pltpu.SMEM(info.shape, I32),
            pltpu.VMEM((requests, heads, dim), BF16),
            pltpu.VMEM(k_rows.shape, BF16),
            pltpu.VMEM(v_rows.shape, BF16),
            pltpu.VMEM(out_weight.shape, BF16),
            pltpu.VMEM((pages, 1, LANES), F32),
            pltpu.VMEM((pages, 1, LANES), F32),
            pltpu.VMEM((n_groups, heads, LANES), F32),
            pltpu.VMEM((n_groups, heads, LANES), F32),
            pltpu.VMEM((n_groups, heads, LANES), F32),
            pltpu.VMEM((n_groups, heads, LANES), F32),
            pltpu.VMEM((sources, rows_here, heads, dim), BF16),
            pltpu.VMEM((sources, heads, LANES), F32),
            pltpu.VMEM((sources, rows_here, heads, dim), BF16),
            pltpu.VMEM((sources, heads, LANES), F32),
            pltpu.VMEM((rows_here * heads, dim), F32),
            pltpu.VMEM((sources, rows_here, width), BF16),
            pltpu.VMEM((nz, requests, columns // nz), BF16),
            pltpu.VMEM((nz, requests, columns // nz), BF16),
            dma,
            dma((3, 4)),
            dma,
            dma,
            dma((sources,)),
            dma((sources,)),
            dma((sources,)),
            dma((sources,)),
            dma((sources,)),
            dma((sources,)),
            dma((sources,)),
            dma((sources,)),
            dma((sources,)),
            dma((sources,)),
            dma((nz,)),
            dma((nz,)),
        ],
        compiler_params=pltpu.CompilerParams(
            vmem_limit_bytes=62 * 1024 * 1024, collective_id=0, has_side_effects=True
        ),
        name="paged",
    )(
        info,
        key_page_scale.T,
        value_page_scale.T,
        queries,
        k_rows,
        v_rows,
        out_weight,
    )


def solution(mesh):
    in_specs = (
        P("req", "head", None),
        P("req", None, "head", None),
        P("req", None, "head", None),
        P("req", "head"),
        P("req", "head"),
        P("req"),
        P("req", None),
        P("head", "req"),
    )
    out_specs = P(None, ("req", "head"))
    return jax.shard_map(
        on_device, mesh=mesh, in_specs=in_specs, out_specs=out_specs, check_vma=False
    )
```

```python
import functools
import math

import jax
import jax.numpy as jnp
from jax import lax
from jax.experimental import pallas as pl
from jax.experimental.pallas import tpu as pltpu
from jax.sharding import PartitionSpec as P

MESH = pl.DeviceIdType.MESH
FLOOR = -1e30
DROP = -3e38
LANES = 128
SUB = 8
LIVE_BITS = 5
ROUND = 8
FIELDS = 16
F32 = jnp.float32
BF16 = jnp.bfloat16
I32 = jnp.int32


def nt(a, b):
    return lax.dot_general(a, b, (((1,), (1,)), ((), ())), preferred_element_type=F32)


def nn(a, b):
    return jnp.dot(a, b, preferred_element_type=F32)


def iota(shape, axis):
    return lax.broadcasted_iota(I32, shape, axis)


def list_kernel(cfg, lengths_ref, table_ref, out_ref):
    sources, rows_here, pages = cfg["sources"], cfg["rows_here"], cfg["pages"]
    page_size, per_group = cfg["page_size"], cfg["per_group"]
    slot_rows, group_rows = cfg["slot_rows"], cfg["group_rows"]
    shape = (rows_here, LANES)
    row_id = iota(shape, 0)
    lengths = jnp.zeros(shape, I32)
    for r in range(rows_here):
        lengths = jnp.where(row_id == r, lengths_ref[r], lengths)
    live = jnp.minimum(lengths - iota(shape, 1) * page_size, page_size)
    table = table_ref[...]
    locals_, mines = [], []
    for d in range(sources):
        local = table - d * pages
        locals_.append(local)
        mines.append((live > 0) & (local >= 0) & (local < pages))
    flag = jnp.concatenate([jnp.where(m, 1.0, 0.0) for m in mines], axis=0).astype(BF16)
    total = sources * rows_here
    up = jnp.where(iota((LANES, LANES), 0) < iota((LANES, LANES), 1), 1.0, 0.0).astype(BF16)
    before = nn(flag, up)
    count = nn(flag, jnp.ones((LANES, LANES), BF16))
    need = jnp.floor((count + (per_group - 1)) * (1.0 / per_group))
    i, j = iota((total, total), 0), iota((total, total), 1)
    tri = jnp.where((i >= j) & (i // rows_here == j // rows_here), 1.0, 0.0).astype(BF16)
    ends = nn(tri, need.astype(BF16))
    starts = ends - need
    slots = (starts * per_group + before).astype(I32)

    key = jnp.full(shape, -1, I32)
    page = jnp.zeros(shape, I32)
    for d in range(sources):
        slot = slots[d * rows_here : (d + 1) * rows_here] + d * (slot_rows * LANES)
        key = jnp.where(mines[d], slot, key)
        page = jnp.where(mines[d], locals_[d], page)
    one = (page >> 2).astype(F32)
    two = ((page & 3) * (1 << LIVE_BITS) + live).astype(F32)
    high, low = key >> 7, key & (LANES - 1)
    hi_rows = -(-(sources * slot_rows) // 16) * 16
    hi_iota, lo_iota = iota((hi_rows, LANES), 0), iota((LANES, LANES), 0)
    lefts, rights = [], []
    for r in range(rows_here):
        row = slice(r, r + 1)
        lefts.append(jnp.where(hi_iota == high[row], 1.0, 0.0).astype(BF16))
        same = lo_iota == low[row]
        pair = [jnp.where(same, one[row], 0.0), jnp.where(same, two[row], 0.0)]
        rights.append(jnp.concatenate(pair, axis=0).astype(BF16))
    found = nt(jnp.concatenate(lefts, axis=1), jnp.concatenate(rights, axis=1))
    found = (found[:, :LANES] * float(4 << LIVE_BITS) + found[:, LANES:]).astype(I32)

    lane = iota(shape, 1).astype(F32)
    diag = row_id == iota(shape, 1)
    for d in range(sources):
        rows = slice(d * rows_here, (d + 1) * rows_here)
        end, begin, some = ends[rows], starts[rows], need[rows] > 0.5
        out_ref[d, :slot_rows, :] = found[d * slot_rows : (d + 1) * slot_rows]
        for b in range(group_rows):
            here = lane + float(b * LANES)
            done = end <= here
            owner = jnp.sum(jnp.where(done, 1.0, 0.0), axis=0, keepdims=True)
            owner = jnp.minimum(owner, float(rows_here - 1))
            last = jnp.min(jnp.where(done, 4096.0, end), axis=0, keepdims=True) - 1.0
            opens = jnp.where((begin == here) & some, 1.0, 0.0)
            opens = jnp.max(opens, axis=0, keepdims=True)
            value = (last * 2.0 + (1.0 - opens)) * float(rows_here) + owner
            out_ref[d, slot_rows + b : slot_rows + b + 1, :] = value.astype(I32)
        mark = jnp.maximum(end - 1.0, 0.0) * 2.0 + jnp.where(some, 1.0, 0.0)
        mark = jnp.sum(jnp.where(diag, mark, 0.0), axis=0, keepdims=True)
        size = jnp.maximum(jnp.max(end, axis=0, keepdims=True), 1.0)
        mark = jnp.where(iota((1, LANES), 1) == rows_here, size, mark)
        base = slot_rows + group_rows
        out_ref[d, base : base + 1, :] = mark.astype(I32)


def kernel(
    cfg,
    info_ref,
    kscale_ref,
    vscale_ref,
    q_hbm,
    k_hbm,
    v_hbm,
    w_hbm,
    out_ref,
    info_all,
    table_vmem,
    table,
    flat,
    q_all,
    k_buf,
    v_buf,
    w_buf,
    kse,
    vse,
    bias,
    scores,
    peaks,
    dens,
    accs,
    pair_send,
    pair_lse_send,
    pair_recv,
    pair_lse_recv,
    num_send,
    lse_send,
    num_recv,
    lse_recv,
    mixed,
    att_all,
    term_send,
    term_recv,
    q_sem,
    load_sems,
    info_sem,
    smem_sem,
    t_send,
    t_recv,
    q_send,
    q_recv,
    q_pass,
    p_send,
    p_recv,
    pl_send,
    pl_recv,
    n_send,
    n_recv,
    l_send,
    l_recv,
    a_send,
    a_recv,
    a_pass,
    z_send,
    z_recv,
):
    sources, nz = cfg["sources"], cfg["nz"]
    rows_here, heads, dim = cfg["rows_here"], cfg["heads"], cfg["dim"]
    pages, page_rows, page_size = cfg["pages"], cfg["page_rows"], cfg["page_size"]
    requests = rows_here * sources
    kv_local = page_rows // page_size
    per_group = LANES // page_rows
    n_groups = cfg["n_groups"]
    steps = n_groups // ROUND
    width = heads * dim
    me = lax.axis_index("req")
    mz = lax.axis_index("head")
    chips = sources // 2
    chip, core = me // 2, lax.rem(me, 2)
    partner = me + 1 - 2 * core

    def other_chip(k):
        return lax.rem(chip + k, chips)

    far = range(chips - 1, 0, -1)
    slot_rows, mark_row = cfg["slot_rows"], cfg["slot_rows"] + cfg["group_rows"]
    last_row = mark_row + cfg["group_rows"]
    per_row = LANES // per_group
    per_row_bits = int(math.log2(per_row))

    q_load = pltpu.make_async_copy(q_hbm, q_all.at[pl.ds(me * rows_here, rows_here)], q_sem)
    q_load.start()
    info_load = pltpu.make_async_copy(info_ref.at[me], info_all.at[me], info_sem)
    info_load.start()
    loads = []
    parts = load_sems.shape[1]
    for which, (src, dst) in enumerate(((k_hbm, k_buf), (v_hbm, v_buf), (w_hbm, w_buf))):
        chunk = src.shape[0] // parts
        for c in range(parts):
            rows = pl.ds(c * chunk, chunk)
            cp = pltpu.make_async_copy(src.at[rows], dst.at[rows], load_sems.at[which, c])
            cp.start()
            loads.append(cp)
    k_loads, v_loads, w_loads = loads[:parts], loads[parts : 2 * parts], loads[2 * parts :]

    barrier = pltpu.get_barrier_semaphore()
    for k in range(1, sources):
        pl.semaphore_signal(
            barrier, inc=1, device_id={"req": lax.rem(me + k, sources)}, device_id_type=MESH
        )
    for k in range(1, nz):
        pl.semaphore_signal(barrier, inc=1, device_id={"head": lax.rem(mz + k, nz)}, device_id_type=MESH)
    pl.semaphore_wait(barrier, sources + nz - 2)

    def info_copy(peer, owner):
        return pltpu.make_async_remote_copy(
            src_ref=info_ref.at[peer],
            dst_ref=info_all.at[owner],
            send_sem=t_send.at[peer],
            recv_sem=t_recv.at[owner],
            device_id={"req": peer},
            device_id_type=MESH,
        )

    def remote(src, dst, send, recv, **where):
        return pltpu.make_async_remote_copy(
            src_ref=src,
            dst_ref=dst,
            send_sem=send,
            recv_sem=recv,
            device_id=where,
            device_id_type=MESH,
        )

    def gather(rows_of, send, recv, passing):
        def direct(peer, owner):
            return remote(rows_of(owner), rows_of(owner), send.at[peer], recv.at[owner], req=peer)

        def onward(owner):
            return remote(rows_of(owner), rows_of(owner), passing.at[owner], recv.at[owner], req=partner)

        def begin():
            for k in far:
                direct(other_chip(k) * 2 + core, me).start()
            direct(partner, me).start()

        def relay():
            for k in far:
                owner = other_chip(k) * 2 + core
                direct(owner, owner).wait_recv()
                onward(owner).start()

        def arrive():
            direct(partner, partner).wait_recv()
            for k in far:
                owner = other_chip(k) * 2 + 1 - core
                onward(owner).wait_recv()

        def finish():
            direct(partner, me).wait_send()
            for k in far:
                owner = other_chip(k) * 2 + core
                direct(owner, me).wait_send()
                onward(owner).wait_send()

        return begin, relay, arrive, finish

    q_begin, q_relay, q_arrive, q_finish = gather(
        lambda owner: q_all.at[pl.ds(owner * rows_here, rows_here)], q_send, q_recv, q_pass
    )
    for k in range(sources - 1, 0, -1):
        info_copy(lax.rem(me + k, sources), me).start()
    q_load.wait()
    q_begin()

    lane_sub = iota((LANES, LANES), 0)
    for src, dst, factor in ((kscale_ref, kse, 1.0 / math.sqrt(dim)), (vscale_ref, vse, 1.0)):
        for b in range(pages // LANES):
            cols = slice(b * LANES, (b + 1) * LANES)
            both = src[kv_local - 1 : kv_local, cols]
            for v in range(kv_local - 1):
                both = jnp.where(lane_sub % kv_local == v, src[v : v + 1, cols], both)
            both = jnp.broadcast_to(both * factor, (LANES, LANES)).T
            dst[b * LANES : (b + 1) * LANES, 0, :] = both

    info_load.wait()
    for k in range(1, sources):
        peer = lax.rem(me + k, sources)
        info_copy(peer, peer).wait_recv()
    for src in range(sources):
        raw = info_all[src]
        value = raw[slot_rows:mark_row]
        table_vmem[src, :slot_rows, :] = raw[:slot_rows] >> LIVE_BITS
        table_vmem[src, slot_rows:mark_row, :] = (value & (rows_here - 1)) + src * rows_here
        table_vmem[src, mark_row : 2 * mark_row - slot_rows, :] = value >> int(math.log2(rows_here))
        table_vmem[src, last_row : last_row + 1, :] = raw[mark_row : mark_row + 1]
    to_smem = pltpu.make_async_copy(table_vmem, table, smem_sem)
    to_smem.start()
    to_smem.wait()

    def flatten(it, at):
        src, k = at
        for j in range(ROUND):
            block = k >> per_row_bits
            column = (k & (per_row - 1)) * per_group
            for i in range(per_group):
                flat[it, j * FIELDS + i] = table[src, block, column + i]
            row, column = k >> 7, k & (LANES - 1)
            flat[it, j * FIELDS + 4] = table[src, slot_rows + row, column]
            last = table[src, mark_row + row, column]
            flat[it, j * FIELDS + 5] = it * ROUND + j - k + (last >> 1)
            flat[it, j * FIELDS + 6] = last & 1
            flat[it, j * FIELDS + 7] = src * (slot_rows * per_row) + k
            more = k + 1 < table[src, last_row, rows_here]
            stay = more | (src + 1 >= sources)
            k = jnp.where(more, k + 1, jnp.where(stay, k, 0))
            src = jnp.where(stay, src, src + 1)
        return src, k

    lax.fori_loop(0, steps, flatten, (jnp.int32(0), jnp.int32(0)))

    spread = jnp.where(iota((LANES, LANES), 0) % per_group == iota((LANES, LANES), 1) // page_rows, 1.0, 0.0)
    spread = spread.astype(BF16)
    chosen = iota((per_row, LANES), 1) // per_group == iota((per_row, LANES), 0)
    token_row = ((iota((1, LANES), 1) % page_rows) // kv_local).astype(F32)
    for src in range(sources):
        live = (info_all[src] & ((1 << LIVE_BITS) - 1)).astype(F32)
        picks = [jnp.where(chosen, live[b : b + 1], 0.0) for b in range(slot_rows)]
        wide = nn(jnp.concatenate(picks, axis=0).astype(BF16), spread)
        rows = slice(src * slot_rows * per_row, (src + 1) * slot_rows * per_row)
        bias[rows, 0, :] = jnp.where(token_row < wide, 0.0, FLOOR)

    q_relay()
    q_arrive()
    for cp in k_loads:
        cp.wait()

    lane8 = iota((SUB, LANES), 1)
    token = (lane8 % page_rows) // kv_local
    per_head = heads // kv_local
    kv_masks = [lane8 % kv_local == (t * SUB) // per_head for t in range(heads // SUB)]
    blank = jnp.zeros((heads, dim), BF16)

    def by_page(parts):
        got = parts[per_group - 1]
        for i in range(per_group - 2, -1, -1):
            got = jnp.where(lane8 < (i + 1) * page_rows, parts[i], got)
        return got

    def fetch(ref, page_ids):
        return jnp.concatenate([ref[p] for p in page_ids], axis=0)

    def scale_row(ref, page_ids):
        return by_page([jnp.broadcast_to(ref[p], (SUB, LANES)) for p in page_ids])

    def same_owner(it, j):
        return jnp.full((heads, LANES), flat[it, j * FIELDS + 6], I32) > 0

    def score_step(it, top):
        for pair in range(ROUND // 2):
            js = (2 * pair, 2 * pair + 1)
            ids = [[flat[it, j * FIELDS + i] for i in range(per_group)] for j in js]
            kk = jnp.concatenate([fetch(k_buf, one) for one in ids], axis=1)
            qa, qb = [q_all[flat[it, j * FIELDS + 4]] for j in js]
            lhs = jnp.concatenate(
                [jnp.concatenate([qa, blank], axis=1), jnp.concatenate([blank, qb], axis=1)], axis=0
            )
            s = nt(lhs, kk)
            for x, j in enumerate(js):
                g = it * ROUND + j
                scale = scale_row(kse, ids[x])
                shift = jnp.broadcast_to(bias[flat[it, j * FIELDS + 7]], (SUB, LANES))
                tiles = []
                for t in range(heads // SUB):
                    tile = s[x * heads + t * SUB : x * heads + (t + 1) * SUB] * scale + shift
                    tiles.append(jnp.where(kv_masks[t], tile, FLOOR))
                tile = jnp.concatenate(tiles, axis=0)
                scores[g] = tile
                mine = jnp.broadcast_to(jnp.max(tile, axis=1, keepdims=True), (heads, LANES))
                top = jnp.where(same_owner(it, j), jnp.maximum(top, mine), mine)
                peaks[g] = top
        return top

    lax.fori_loop(0, steps, score_step, jnp.full((heads, LANES), FLOOR, F32))
    for cp in v_loads:
        cp.wait()

    def value_step(it, carry):
        acc, den = carry
        for pair in range(ROUND // 2):
            js = (2 * pair, 2 * pair + 1)
            ids = [[flat[it, j * FIELDS + i] for i in range(per_group)] for j in js]
            vv = jnp.concatenate([fetch(v_buf, one) for one in ids], axis=1)
            lhs, weights = [], []
            for x, j in enumerate(js):
                weight = jnp.exp(scores[it * ROUND + j] - peaks[flat[it, j * FIELDS + 5]])
                scale = scale_row(vse, ids[x])
                scaled = [weight[t * SUB : (t + 1) * SUB] * scale for t in range(heads // SUB)]
                lhs.append(jnp.concatenate(scaled, axis=0).astype(BF16))
                weights.append(weight)
            o = nn(jnp.concatenate(lhs, axis=0), vv)
            for x, j in enumerate(js):
                g = it * ROUND + j
                keep = same_owner(it, j)
                mine = o[x * heads : (x + 1) * heads, x * dim : (x + 1) * dim]
                acc = jnp.where(keep, acc + mine, mine)
                den = jnp.where(keep, den + weights[x], weights[x])
                accs[g] = acc
                dens[g] = den
        return acc, den

    zero = jnp.zeros((heads, LANES), F32)
    lax.fori_loop(0, steps, value_step, (zero, zero))

    lane16 = iota((heads, LANES), 1)

    def first_group(dest):
        base = jnp.int32(0)
        for src in range(sources):
            base = base + jnp.where(src < dest, table[src, last_row, rows_here], 0)
        return base

    def local_part(dest, base, r):
        mark = table[dest, last_row, r]
        last = base + (mark >> 1)
        some = (mark & 1).astype(F32)
        den = jnp.broadcast_to(jnp.sum(dens[last], axis=1, keepdims=True), (heads, LANES))
        den = jnp.maximum(den, 0.5)
        num = accs[last] * (some / den)
        return num, (peaks[last] + jnp.log(den)) * some + (some - 1.0) * (-FLOOR)

    def pair_copy(c):
        return remote(pair_send.at[c], pair_recv.at[c], p_send.at[c], p_recv.at[c], req=partner)

    def pair_lse_copy(c):
        return remote(pair_lse_send.at[c], pair_lse_recv.at[c], pl_send.at[c], pl_recv.at[c], req=partner)

    def num_copy(to, owner):
        return remote(
            num_send.at[to], num_recv.at[owner], n_send.at[to], n_recv.at[owner], req=to * 2 + core
        )

    def lse_copy(to, owner):
        return remote(
            lse_send.at[to], lse_recv.at[owner], l_send.at[to], l_recv.at[owner], req=to * 2 + core
        )

    def for_partner(k, carry):
        c = other_chip(chips - 1 - k)
        dest = c * 2 + 1 - core
        base = first_group(dest)
        tile = jnp.full((heads, LANES), FLOOR, F32)
        for r in range(rows_here):
            num, lse = local_part(dest, base, r)
            pair_send[c, r] = num.astype(BF16)
            tile = jnp.where(lane16 == r, lse, tile)
        pair_lse_send[c] = tile
        pair_copy(c).start()
        pair_lse_copy(c).start()
        return carry

    lax.fori_loop(0, chips, for_partner, 0)

    def merge(c, num_at, lse_at):
        dest = c * 2 + core
        base = first_group(dest)
        theirs = pair_lse_recv[c]
        tile = jnp.full((heads, LANES), FLOOR, F32)
        for r in range(rows_here):
            num, lse = local_part(dest, base, r)
            their = jnp.broadcast_to(theirs[:, r : r + 1], (heads, LANES))
            high = jnp.maximum(lse, their)
            a, b = jnp.exp(lse - high), jnp.exp(their - high)
            total = a + b
            got = (num * a + pair_recv[c, r].astype(F32) * b) / total
            num_at[r] = got.astype(BF16)
            tile = jnp.where(lane16 == r, high + jnp.log(total), tile)
        lse_at[...] = tile

    def send_block(k, carry):
        c = other_chip(chips - 1 - k)
        merge(c, num_send.at[c], lse_send.at[c])
        num_copy(c, chip).start()
        lse_copy(c, chip).start()
        return carry

    for k in range(chips - 1, -1, -1):
        pair_lse_copy(other_chip(k)).wait_recv()
        pair_copy(other_chip(k)).wait_recv()
    lax.fori_loop(0, chips - 1, send_block, 0)
    merge(chip, num_recv.at[chip], lse_recv.at[chip])
    for k in far:
        c = other_chip(k)
        lse_copy(c, c).wait_recv()
        num_copy(c, c).wait_recv()

    lses = [lse_recv[s] for s in range(chips)]
    top = functools.reduce(jnp.maximum, lses)
    shares = [jnp.exp(x - top) for x in lses]
    total = functools.reduce(jnp.add, shares)
    shares = [x / total for x in shares]
    for r in range(rows_here):
        got = jnp.zeros((heads, dim), F32)
        for s in range(chips):
            share = jnp.broadcast_to(shares[s][:, r : r + 1], (heads, dim))
            got = got + share * num_recv[s, r].astype(F32)
        mixed[r * heads : (r + 1) * heads, :] = got
    for h in range(heads):
        rows = mixed[pl.ds(h, rows_here, stride=heads), :]
        att_all[me, :, h * dim : (h + 1) * dim] = rows.astype(BF16)

    a_begin, a_relay, a_arrive, a_finish = gather(lambda owner: att_all.at[owner], a_send, a_recv, a_pass)
    a_begin()
    for cp in w_loads:
        cp.wait()
    a_relay()
    a_arrive()

    att = att_all[...].reshape(requests, width)
    cols = w_buf.shape[1] // nz

    def term_copy(peer, owner):
        return pltpu.make_async_remote_copy(
            src_ref=term_send.at[peer],
            dst_ref=term_recv.at[owner],
            send_sem=z_send.at[peer],
            recv_sem=z_recv.at[owner],
            device_id={"head": peer},
            device_id_type=MESH,
        )

    def project(z):
        return nn(att, w_buf[:, pl.ds(pl.multiple_of(z * cols, cols), cols)])

    if cols % LANES == 0:
        for k in range(1, nz):
            peer = lax.rem(mz + k, nz)
            term_send[peer] = project(peer).astype(BF16)
            term_copy(peer, mz).start()
        result = project(mz)
    else:
        every = nn(att, w_buf[...])
        for z in range(nz):
            term_send[z] = every[:, z * cols : (z + 1) * cols].astype(BF16)
        for k in range(1, nz):
            term_copy(lax.rem(mz + k, nz), mz).start()
        result = term_send[mz].astype(F32)
    for k in range(1, nz):
        peer = lax.rem(mz + k, nz)
        term_copy(peer, peer).wait_recv()
        result = result + term_recv[peer].astype(F32)
    out_ref[...] = result.astype(BF16)

    for k in range(1, sources):
        peer = lax.rem(me + k, sources)
        info_copy(peer, me).wait_send()
    q_finish()
    a_finish()
    for c in range(chips):
        pair_copy(c).wait_send()
        pair_lse_copy(c).wait_send()
    for k in far:
        c = other_chip(k)
        num_copy(c, chip).wait_send()
        lse_copy(c, chip).wait_send()
    for k in range(1, nz):
        term_copy(lax.rem(mz + k, nz), mz).wait_send()


def on_device(
    queries,
    k_codes,
    value_quantized_codes,
    key_page_scale,
    value_page_scale,
    lengths,
    page_table,
    out_weight,
):
    pages, page_size, kv_local, dim = k_codes.shape
    rows_here, heads, _ = queries.shape
    sources, nz = lax.axis_size("req"), lax.axis_size("head")
    requests = rows_here * sources
    page_rows = page_size * kv_local
    per_group = LANES // page_rows
    group_bound = (pages + (per_group - 1) * requests) // per_group + sources
    n_groups = -(-group_bound // ROUND) * ROUND
    list_bound = (pages + (per_group - 1) * rows_here) // per_group
    slot_rows = -(-list_bound * per_group // LANES)
    group_rows = -(-list_bound // LANES)
    info_rows = -(-(slot_rows + group_rows + 1) // SUB) * SUB
    table_rows = -(-(slot_rows + 2 * group_rows + 1) // SUB) * SUB
    chips = sources // 2
    k_rows = k_codes.reshape(pages, page_rows, dim)
    v_rows = value_quantized_codes.reshape(pages, page_rows, dim)
    width = heads * dim
    columns = out_weight.shape[1]
    cfg = dict(
        sources=sources,
        nz=nz,
        rows_here=rows_here,
        heads=heads,
        dim=dim,
        pages=pages,
        page_rows=page_rows,
        page_size=page_size,
        n_groups=n_groups,
        per_group=per_group,
        slot_rows=slot_rows,
        group_rows=group_rows,
    )
    vmem = pl.BlockSpec(memory_space=pltpu.VMEM)
    smem = pl.BlockSpec(memory_space=pltpu.SMEM)
    hbm = pl.BlockSpec(memory_space=pl.ANY)
    dma = pltpu.SemaphoreType.DMA
    info = pl.pallas_call(
        functools.partial(list_kernel, cfg),
        out_shape=jax.ShapeDtypeStruct((sources, info_rows, LANES), I32),
        in_specs=[smem, vmem],
        out_specs=vmem,
        name="lists",
    )(lengths, page_table)
    return pl.pallas_call(
        functools.partial(kernel, cfg),
        out_shape=jax.ShapeDtypeStruct((requests, columns // nz), BF16),
        in_specs=[vmem, vmem, vmem, hbm, hbm, hbm, hbm],
        out_specs=vmem,
        scratch_shapes=[
            pltpu.VMEM(info.shape, I32),
            pltpu.VMEM((sources, table_rows, LANES), I32),
            pltpu.SMEM((sources, table_rows, LANES), I32),
            pltpu.SMEM((n_groups // ROUND, LANES), I32),
            pltpu.VMEM((requests, heads, dim), BF16),
            pltpu.VMEM(k_rows.shape, BF16),
            pltpu.VMEM(v_rows.shape, BF16),
            pltpu.VMEM(out_weight.shape, BF16),
            pltpu.VMEM((pages, 1, LANES), F32),
            pltpu.VMEM((pages, 1, LANES), F32),
            pltpu.VMEM((sources * slot_rows * (LANES // per_group), 1, LANES), F32),
            pltpu.VMEM((n_groups, heads, LANES), F32),
            pltpu.VMEM((n_groups, heads, LANES), F32),
            pltpu.VMEM((n_groups, heads, LANES), F32),
            pltpu.VMEM((n_groups, heads, LANES), F32),
            pltpu.VMEM((chips, rows_here, heads, dim), BF16),
            pltpu.VMEM((chips, heads, LANES), F32),
            pltpu.VMEM((chips, rows_here, heads, dim), BF16),
            pltpu.VMEM((chips, heads, LANES), F32),
            pltpu.VMEM((chips, rows_here, heads, dim), BF16),
            pltpu.VMEM((chips, heads, LANES), F32),
            pltpu.VMEM((chips, rows_here, heads, dim), BF16),
            pltpu.VMEM((chips, heads, LANES), F32),
            pltpu.VMEM((rows_here * heads, dim), F32),
            pltpu.VMEM((sources, rows_here, width), BF16),
            pltpu.VMEM((nz, requests, columns // nz), BF16),
            pltpu.VMEM((nz, requests, columns // nz), BF16),
            dma,
            dma((3, 4)),
            dma,
            dma,
            dma((sources,)),
            dma((sources,)),
            dma((sources,)),
            dma((sources,)),
            dma((sources,)),
            dma((chips,)),
            dma((chips,)),
            dma((chips,)),
            dma((chips,)),
            dma((chips,)),
            dma((chips,)),
            dma((chips,)),
            dma((chips,)),
            dma((sources,)),
            dma((sources,)),
            dma((sources,)),
            dma((nz,)),
            dma((nz,)),
        ],
        compiler_params=pltpu.CompilerParams(
            vmem_limit_bytes=62 * 1024 * 1024, collective_id=0, has_side_effects=True
        ),
        name="paged",
    )(
        info,
        key_page_scale.T,
        value_page_scale.T,
        queries,
        k_rows,
        v_rows,
        out_weight,
    )


def solution(mesh):
    in_specs = (
        P("req", "head", None),
        P("req", None, "head", None),
        P("req", None, "head", None),
        P("req", "head"),
        P("req", "head"),
        P("req"),
        P("req", None),
        P("head", "req"),
    )
    out_specs = P(None, ("req", "head"))
    return jax.shard_map(
        on_device, mesh=mesh, in_specs=in_specs, out_specs=out_specs, check_vma=False
    )
```

```python
import functools
import math

import jax
import jax.numpy as jnp
from jax import lax
from jax.experimental import pallas as pl
from jax.experimental.pallas import tpu as pltpu
from jax.sharding import PartitionSpec as P

MESH = pl.DeviceIdType.MESH
FLOOR = -1e30
DROP = -3e38
LANES = 128
SUB = 8
LIVE_BITS = 5
OWNER_SHIFT = 7
FIELDS = 8
ROUND = LANES // FIELDS
F32 = jnp.float32
BF16 = jnp.bfloat16
I32 = jnp.int32


def nt(a, b):
    return lax.dot_general(a, b, (((1,), (1,)), ((), ())), preferred_element_type=F32)


def nn(a, b):
    return jnp.dot(a, b, preferred_element_type=F32)


def iota(shape, axis):
    return lax.broadcasted_iota(I32, shape, axis)


def list_kernel(cfg, lengths_ref, table_ref, out_ref):
    sources, rows_here, pages = cfg["sources"], cfg["rows_here"], cfg["pages"]
    page_size, per_group = cfg["page_size"], cfg["per_group"]
    list_rows = cfg["list_rows"]
    shape = (rows_here, LANES)
    row_id = iota(shape, 0)
    lengths = jnp.zeros(shape, I32)
    for r in range(rows_here):
        lengths = jnp.where(row_id == r, lengths_ref[r], lengths)
    live = jnp.minimum(lengths - iota(shape, 1) * page_size, page_size)
    table = table_ref[...]
    locals_, mines = [], []
    for d in range(sources):
        local = table - d * pages
        locals_.append(local)
        mines.append((live > 0) & (local >= 0) & (local < pages))
    flag = jnp.concatenate([jnp.where(m, 1.0, 0.0) for m in mines], axis=0).astype(BF16)
    total = sources * rows_here
    up = jnp.where(iota((LANES, LANES), 0) < iota((LANES, LANES), 1), 1.0, 0.0).astype(BF16)
    before = nn(flag, up)
    count = nn(flag, jnp.ones((LANES, LANES), BF16))
    need = jnp.floor((count + (per_group - 1)) * (1.0 / per_group))
    i, j = iota((total, total), 0), iota((total, total), 1)
    tri = jnp.where((i >= j) & (i // rows_here == j // rows_here), 1.0, 0.0).astype(BF16)
    ends = nn(tri, need.astype(BF16))
    starts = ends - need
    before, starts_int, need_int = before.astype(I32), starts.astype(I32), need.astype(I32)

    high = jnp.full(shape, -1, I32)
    low, lead, page, rest = high, high, high, high
    for d in range(sources):
        rows = slice(d * rows_here, (d + 1) * rows_here)
        step = before[rows] >> 2
        group = starts_int[rows] + step
        column = (group & (ROUND - 1)) * FIELDS
        place = before[rows] & 3
        high = jnp.where(mines[d], d * list_rows + group // ROUND, high)
        low = jnp.where(mines[d], column + place, low)
        lead = jnp.where(mines[d] & (place == 0), column + per_group, lead)
        page = jnp.where(mines[d], locals_[d], page)
        left = (need_int[rows] - 1 - step) * 2 + jnp.where(step == 0, 1, 0)
        rest = jnp.where(mines[d], left, rest)
    one = (page >> 2).astype(F32)
    two = ((page & 3) * (1 << LIVE_BITS) + live).astype(F32)
    rest = rest.astype(F32)
    hi_rows = -(-(sources * list_rows) // 16) * 16
    hi_iota, lo_iota = iota((hi_rows, LANES), 0), iota((LANES, LANES), 0)
    lefts, rights = [], []
    for r in range(rows_here):
        row = slice(r, r + 1)
        lefts.append(jnp.where(hi_iota == high[row], 1.0, 0.0).astype(BF16))
        same, head = lo_iota == low[row], lo_iota == lead[row]
        pair = [
            jnp.where(same, one[row], jnp.where(head, float(r), 0.0)),
            jnp.where(same, two[row], jnp.where(head, rest[row], 0.0)),
        ]
        rights.append(jnp.concatenate(pair, axis=0).astype(BF16))
    found = nt(jnp.concatenate(lefts, axis=1), jnp.concatenate(rights, axis=1))
    found = (found[:, :LANES] * float(4 << LIVE_BITS) + found[:, LANES:]).astype(I32)

    diag = row_id == iota(shape, 1)
    for d in range(sources):
        rows = slice(d * rows_here, (d + 1) * rows_here)
        end, some = ends[rows], need[rows] > 0.5
        out_ref[d, :list_rows, :] = found[d * list_rows : (d + 1) * list_rows]
        mark = jnp.maximum(end - 1.0, 0.0) * 2.0 + jnp.where(some, 1.0, 0.0)
        mark = jnp.sum(jnp.where(diag, mark, 0.0), axis=0, keepdims=True)
        size = jnp.max(end, axis=0, keepdims=True)
        mark = jnp.where(iota((1, LANES), 1) == rows_here, size, mark)
        out_ref[d, list_rows : list_rows + 1, :] = mark.astype(I32)


def kernel(
    cfg,
    info_ref,
    kscale_ref,
    vscale_ref,
    q_hbm,
    k_hbm,
    v_hbm,
    w_hbm,
    out_ref,
    info_all,
    mark_vmem,
    marks,
    flat_vmem,
    flat,
    q_all,
    k_buf,
    v_buf,
    w_buf,
    kse,
    vse,
    bias,
    scores,
    peaks,
    dens,
    accs,
    pair_send,
    pair_lse_send,
    pair_recv,
    pair_lse_recv,
    num_send,
    lse_send,
    num_recv,
    lse_recv,
    mixed,
    att_all,
    term_send,
    term_recv,
    q_sem,
    load_sems,
    info_sem,
    mark_sem,
    flat_sem,
    t_send,
    t_recv,
    q_send,
    q_recv,
    q_pass,
    p_send,
    p_recv,
    pl_send,
    pl_recv,
    n_send,
    n_recv,
    l_send,
    l_recv,
    a_send,
    a_recv,
    a_pass,
    z_send,
    z_recv,
):
    sources, nz = cfg["sources"], cfg["nz"]
    rows_here, heads, dim = cfg["rows_here"], cfg["heads"], cfg["dim"]
    pages, page_rows, page_size = cfg["pages"], cfg["page_rows"], cfg["page_size"]
    requests = rows_here * sources
    kv_local = page_rows // page_size
    per_group = LANES // page_rows
    n_groups = cfg["n_groups"]
    steps = n_groups // ROUND
    width = heads * dim
    me = lax.axis_index("req")
    mz = lax.axis_index("head")
    chips = sources // 2
    chip, core = me // 2, lax.rem(me, 2)
    partner = me + 1 - 2 * core

    def other_chip(k):
        return lax.rem(chip + k, chips)

    far = range(chips - 1, 0, -1)
    list_rows = cfg["list_rows"]
    flat_rows = flat_vmem.shape[0]

    q_load = pltpu.make_async_copy(q_hbm, q_all.at[pl.ds(me * rows_here, rows_here)], q_sem)
    q_load.start()
    info_load = pltpu.make_async_copy(info_ref.at[me], info_all.at[me], info_sem)
    info_load.start()
    loads = []
    parts = load_sems.shape[1]
    for which, (src, dst) in enumerate(((k_hbm, k_buf), (v_hbm, v_buf), (w_hbm, w_buf))):
        chunk = src.shape[0] // parts
        for c in range(parts):
            rows = pl.ds(c * chunk, chunk)
            cp = pltpu.make_async_copy(src.at[rows], dst.at[rows], load_sems.at[which, c])
            cp.start()
            loads.append(cp)
    k_loads, v_loads, w_loads = loads[:parts], loads[parts : 2 * parts], loads[2 * parts :]

    barrier = pltpu.get_barrier_semaphore()
    for k in range(1, sources):
        pl.semaphore_signal(
            barrier, inc=1, device_id={"req": lax.rem(me + k, sources)}, device_id_type=MESH
        )
    for k in range(1, nz):
        pl.semaphore_signal(barrier, inc=1, device_id={"head": lax.rem(mz + k, nz)}, device_id_type=MESH)
    pl.semaphore_wait(barrier, sources + nz - 2)

    def info_copy(peer, owner):
        return pltpu.make_async_remote_copy(
            src_ref=info_ref.at[peer],
            dst_ref=info_all.at[owner],
            send_sem=t_send.at[peer],
            recv_sem=t_recv.at[owner],
            device_id={"req": peer},
            device_id_type=MESH,
        )

    def remote(src, dst, send, recv, **where):
        return pltpu.make_async_remote_copy(
            src_ref=src,
            dst_ref=dst,
            send_sem=send,
            recv_sem=recv,
            device_id=where,
            device_id_type=MESH,
        )

    def gather(rows_of, send, recv, passing):
        def direct(peer, owner):
            return remote(rows_of(owner), rows_of(owner), send.at[peer], recv.at[owner], req=peer)

        def onward(owner):
            return remote(rows_of(owner), rows_of(owner), passing.at[owner], recv.at[owner], req=partner)

        def begin():
            for k in far:
                direct(other_chip(k) * 2 + core, me).start()
            direct(partner, me).start()

        def relay():
            for k in far:
                owner = other_chip(k) * 2 + core
                direct(owner, owner).wait_recv()
                onward(owner).start()

        def arrive():
            direct(partner, partner).wait_recv()
            for k in far:
                owner = other_chip(k) * 2 + 1 - core
                onward(owner).wait_recv()

        def finish():
            direct(partner, me).wait_send()
            for k in far:
                owner = other_chip(k) * 2 + core
                direct(owner, me).wait_send()
                onward(owner).wait_send()

        return begin, relay, arrive, finish

    q_begin, q_relay, q_arrive, q_finish = gather(
        lambda owner: q_all.at[pl.ds(owner * rows_here, rows_here)], q_send, q_recv, q_pass
    )
    for k in range(sources - 1, 0, -1):
        info_copy(lax.rem(me + k, sources), me).start()
    q_load.wait()
    q_begin()

    lane_sub = iota((LANES, LANES), 0)
    for src, dst, factor in ((kscale_ref, kse, 1.0 / math.sqrt(dim)), (vscale_ref, vse, 1.0)):
        for b in range(pages // LANES):
            cols = slice(b * LANES, (b + 1) * LANES)
            both = src[kv_local - 1 : kv_local, cols]
            for v in range(kv_local - 1):
                both = jnp.where(lane_sub % kv_local == v, src[v : v + 1, cols], both)
            both = jnp.broadcast_to(both * factor, (LANES, LANES)).T
            dst[b * LANES : (b + 1) * LANES, 0, :] = both

    info_load.wait()
    for k in range(1, sources):
        peer = lax.rem(me + k, sources)
        info_copy(peer, peer).wait_recv()
    for src in range(sources):
        mark_vmem[src : src + 1, :] = info_all[src, list_rows : list_rows + 1, :]
    to_smem = pltpu.make_async_copy(mark_vmem, marks, mark_sem)
    to_smem.start()
    to_smem.wait()

    shape = (flat_rows, LANES)
    lane, field = iota(shape, 1), iota(shape, 1) % FIELDS
    group = iota(shape, 0) * ROUND + lane // FIELDS
    joined = jnp.zeros(shape, I32)
    base = jnp.int32(0)
    for src in range(sources):
        size = marks[src, rows_here]
        rows = min(flat_rows, info_all.shape[1])
        one = info_all[src, :rows, :]
        if rows < flat_rows:
            one = jnp.concatenate([one, jnp.zeros((flat_rows - rows, LANES), I32)], axis=0)
        one = jnp.where(field == per_group, one + (src * rows_here << OWNER_SHIFT), one)
        move = (base & (ROUND - 1)) * FIELDS
        one = pltpu.roll(one, move, axis=1)
        one = jnp.where(lane < move, pltpu.roll(one, 1, axis=0), one)
        one = pltpu.roll(one, base // ROUND, axis=0)
        joined = jnp.where((group >= base) & (group < base + size), one, joined)
        base = base + size
    low_bits = (1 << OWNER_SHIFT) - 1
    last = group + ((pltpu.roll(joined, 1, axis=1) & low_bits) >> 1)
    fresh = pltpu.roll(joined, 2, axis=1) & 1
    values = jnp.where(field == per_group + 1, last, fresh)
    values = jnp.where(field == per_group, joined >> OWNER_SHIFT, values)
    flat_vmem[...] = jnp.where(field < per_group, joined >> LIVE_BITS, values)
    to_smem = pltpu.make_async_copy(flat_vmem, flat, flat_sem)
    to_smem.start()

    live = jnp.where(field < per_group, joined & ((1 << LIVE_BITS) - 1), 0).astype(F32)
    spread = iota((LANES, LANES), 0) % FIELDS == iota((LANES, LANES), 1) // page_rows
    spread = jnp.where(spread, 1.0, 0.0).astype(BF16)
    chosen = iota((ROUND, LANES), 1) // FIELDS == iota((ROUND, LANES), 0)
    token_row = ((iota((1, LANES), 1) % page_rows) // kv_local).astype(F32)
    picks = [jnp.where(chosen, live[b : b + 1], 0.0) for b in range(steps)]
    wide = nn(jnp.concatenate(picks, axis=0).astype(BF16), spread)
    bias[:, 0, :] = jnp.where(token_row < wide, 0.0, FLOOR)
    to_smem.wait()

    q_relay()
    q_arrive()
    for cp in k_loads:
        cp.wait()

    lane8 = iota((SUB, LANES), 1)
    token = (lane8 % page_rows) // kv_local
    per_head = heads // kv_local
    kv_masks = [lane8 % kv_local == (t * SUB) // per_head for t in range(heads // SUB)]
    blank = jnp.zeros((heads, dim), BF16)

    def by_page(parts):
        got = parts[per_group - 1]
        for i in range(per_group - 2, -1, -1):
            got = jnp.where(lane8 < (i + 1) * page_rows, parts[i], got)
        return got

    def fetch(ref, page_ids):
        return jnp.concatenate([ref[p] for p in page_ids], axis=0)

    def scale_row(ref, page_ids):
        return by_page([jnp.broadcast_to(ref[p], (SUB, LANES)) for p in page_ids])

    def same_owner(it, j):
        return jnp.full((heads, LANES), flat[it, j * FIELDS + per_group + 2], I32) == 0

    def score_step(it, top):
        for pair in range(ROUND // 2):
            js = (2 * pair, 2 * pair + 1)
            ids = [[flat[it, j * FIELDS + i] for i in range(per_group)] for j in js]
            kk = jnp.concatenate([fetch(k_buf, one) for one in ids], axis=1)
            qa, qb = [q_all[flat[it, j * FIELDS + per_group]] for j in js]
            lhs = jnp.concatenate(
                [jnp.concatenate([qa, blank], axis=1), jnp.concatenate([blank, qb], axis=1)], axis=0
            )
            s = nt(lhs, kk)
            for x, j in enumerate(js):
                g = it * ROUND + j
                scale = scale_row(kse, ids[x])
                shift = jnp.broadcast_to(bias[g], (SUB, LANES))
                tiles = []
                for t in range(heads // SUB):
                    tile = s[x * heads + t * SUB : x * heads + (t + 1) * SUB] * scale + shift
                    tiles.append(jnp.where(kv_masks[t], tile, FLOOR))
                tile = jnp.concatenate(tiles, axis=0)
                scores[g] = tile
                mine = jnp.broadcast_to(jnp.max(tile, axis=1, keepdims=True), (heads, LANES))
                top = jnp.where(same_owner(it, j), jnp.maximum(top, mine), mine)
                peaks[g] = top
        return top

    lax.fori_loop(0, steps, score_step, jnp.full((heads, LANES), FLOOR, F32))
    for cp in v_loads:
        cp.wait()

    def value_step(it, carry):
        acc, den = carry
        for pair in range(ROUND // 2):
            js = (2 * pair, 2 * pair + 1)
            ids = [[flat[it, j * FIELDS + i] for i in range(per_group)] for j in js]
            vv = jnp.concatenate([fetch(v_buf, one) for one in ids], axis=1)
            lhs, weights = [], []
            for x, j in enumerate(js):
                weight = jnp.exp(scores[it * ROUND + j] - peaks[flat[it, j * FIELDS + per_group + 1]])
                scale = scale_row(vse, ids[x])
                scaled = [weight[t * SUB : (t + 1) * SUB] * scale for t in range(heads // SUB)]
                lhs.append(jnp.concatenate(scaled, axis=0).astype(BF16))
                weights.append(weight)
            o = nn(jnp.concatenate(lhs, axis=0), vv)
            for x, j in enumerate(js):
                g = it * ROUND + j
                keep = same_owner(it, j)
                mine = o[x * heads : (x + 1) * heads, x * dim : (x + 1) * dim]
                acc = jnp.where(keep, acc + mine, mine)
                den = jnp.where(keep, den + weights[x], weights[x])
                accs[g] = acc
                dens[g] = den
        return acc, den

    zero = jnp.zeros((heads, LANES), F32)
    lax.fori_loop(0, steps, value_step, (zero, zero))

    lane16 = iota((heads, LANES), 1)

    def first_group(dest):
        base = jnp.int32(0)
        for src in range(sources):
            base = base + jnp.where(src < dest, marks[src, rows_here], 0)
        return base

    def local_part(dest, base, r):
        mark = marks[dest, r]
        last = base + (mark >> 1)
        some = (mark & 1).astype(F32)
        den = jnp.broadcast_to(jnp.sum(dens[last], axis=1, keepdims=True), (heads, LANES))
        den = jnp.maximum(den, 0.5)
        num = accs[last] * (some / den)
        return num, (peaks[last] + jnp.log(den)) * some + (some - 1.0) * (-FLOOR)

    def pair_copy(c):
        return remote(pair_send.at[c], pair_recv.at[c], p_send.at[c], p_recv.at[c], req=partner)

    def pair_lse_copy(c):
        return remote(pair_lse_send.at[c], pair_lse_recv.at[c], pl_send.at[c], pl_recv.at[c], req=partner)

    def num_copy(to, owner):
        return remote(
            num_send.at[to], num_recv.at[owner], n_send.at[to], n_recv.at[owner], req=to * 2 + core
        )

    def lse_copy(to, owner):
        return remote(
            lse_send.at[to], lse_recv.at[owner], l_send.at[to], l_recv.at[owner], req=to * 2 + core
        )

    def for_partner(k, carry):
        c = other_chip(chips - 1 - k)
        dest = c * 2 + 1 - core
        base = first_group(dest)
        tile = jnp.full((heads, LANES), FLOOR, F32)
        for r in range(rows_here):
            num, lse = local_part(dest, base, r)
            pair_send[c, r] = num.astype(BF16)
            tile = jnp.where(lane16 == r, lse, tile)
        pair_lse_send[c] = tile
        pair_copy(c).start()
        pair_lse_copy(c).start()
        return carry

    lax.fori_loop(0, chips, for_partner, 0)

    def merge(c, num_at, lse_at):
        dest = c * 2 + core
        base = first_group(dest)
        theirs = pair_lse_recv[c]
        tile = jnp.full((heads, LANES), FLOOR, F32)
        for r in range(rows_here):
            num, lse = local_part(dest, base, r)
            their = jnp.broadcast_to(theirs[:, r : r + 1], (heads, LANES))
            high = jnp.maximum(lse, their)
            a, b = jnp.exp(lse - high), jnp.exp(their - high)
            total = a + b
            got = (num * a + pair_recv[c, r].astype(F32) * b) / total
            num_at[r] = got.astype(BF16)
            tile = jnp.where(lane16 == r, high + jnp.log(total), tile)
        lse_at[...] = tile

    def send_block(k, carry):
        c = other_chip(chips - 1 - k)
        merge(c, num_send.at[c], lse_send.at[c])
        num_copy(c, chip).start()
        lse_copy(c, chip).start()
        return carry

    for k in range(chips - 1, -1, -1):
        pair_lse_copy(other_chip(k)).wait_recv()
        pair_copy(other_chip(k)).wait_recv()
    lax.fori_loop(0, chips - 1, send_block, 0)
    merge(chip, num_recv.at[chip], lse_recv.at[chip])
    for k in far:
        c = other_chip(k)
        lse_copy(c, c).wait_recv()
        num_copy(c, c).wait_recv()

    lses = [lse_recv[s] for s in range(chips)]
    top = functools.reduce(jnp.maximum, lses)
    shares = [jnp.exp(x - top) for x in lses]
    total = functools.reduce(jnp.add, shares)
    shares = [x / total for x in shares]
    for r in range(rows_here):
        got = jnp.zeros((heads, dim), F32)
        for s in range(chips):
            share = jnp.broadcast_to(shares[s][:, r : r + 1], (heads, dim))
            got = got + share * num_recv[s, r].astype(F32)
        mixed[r * heads : (r + 1) * heads, :] = got
    for h in range(heads):
        rows = mixed[pl.ds(h, rows_here, stride=heads), :]
        att_all[me, :, h * dim : (h + 1) * dim] = rows.astype(BF16)

    a_begin, a_relay, a_arrive, a_finish = gather(lambda owner: att_all.at[owner], a_send, a_recv, a_pass)
    a_begin()
    for cp in w_loads:
        cp.wait()
    a_relay()
    a_arrive()

    att = att_all[...].reshape(requests, width)
    cols = w_buf.shape[1] // nz

    def term_copy(peer, owner):
        return pltpu.make_async_remote_copy(
            src_ref=term_send.at[peer],
            dst_ref=term_recv.at[owner],
            send_sem=z_send.at[peer],
            recv_sem=z_recv.at[owner],
            device_id={"head": peer},
            device_id_type=MESH,
        )

    def project(z):
        return nn(att, w_buf[:, pl.ds(pl.multiple_of(z * cols, cols), cols)])

    if cols % LANES == 0:
        for k in range(1, nz):
            peer = lax.rem(mz + k, nz)
            term_send[peer] = project(peer).astype(BF16)
            term_copy(peer, mz).start()
        result = project(mz)
    else:
        every = nn(att, w_buf[...])
        for z in range(nz):
            term_send[z] = every[:, z * cols : (z + 1) * cols].astype(BF16)
        for k in range(1, nz):
            term_copy(lax.rem(mz + k, nz), mz).start()
        result = term_send[mz].astype(F32)
    for k in range(1, nz):
        peer = lax.rem(mz + k, nz)
        term_copy(peer, peer).wait_recv()
        result = result + term_recv[peer].astype(F32)
    out_ref[...] = result.astype(BF16)

    for k in range(1, sources):
        peer = lax.rem(me + k, sources)
        info_copy(peer, me).wait_send()
    q_finish()
    a_finish()
    for c in range(chips):
        pair_copy(c).wait_send()
        pair_lse_copy(c).wait_send()
    for k in far:
        c = other_chip(k)
        num_copy(c, chip).wait_send()
        lse_copy(c, chip).wait_send()
    for k in range(1, nz):
        term_copy(lax.rem(mz + k, nz), mz).wait_send()


def on_device(
    queries,
    k_codes,
    value_quantized_codes,
    key_page_scale,
    value_page_scale,
    lengths,
    page_table,
    out_weight,
):
    pages, page_size, kv_local, dim = k_codes.shape
    rows_here, heads, _ = queries.shape
    sources, nz = lax.axis_size("req"), lax.axis_size("head")
    requests = rows_here * sources
    page_rows = page_size * kv_local
    per_group = LANES // page_rows
    group_bound = (pages + (per_group - 1) * requests) // per_group
    n_groups = -(-group_bound // ROUND) * ROUND
    list_bound = (pages + (per_group - 1) * rows_here) // per_group
    list_rows = -(-list_bound // ROUND)
    info_rows = -(-(list_rows + 1) // SUB) * SUB
    flat_rows = -(-(n_groups // ROUND) // SUB) * SUB
    mark_rows = -(-sources // SUB) * SUB
    chips = sources // 2
    k_rows = k_codes.reshape(pages, page_rows, dim)
    v_rows = value_quantized_codes.reshape(pages, page_rows, dim)
    width = heads * dim
    columns = out_weight.shape[1]
    cfg = dict(
        sources=sources,
        nz=nz,
        rows_here=rows_here,
        heads=heads,
        dim=dim,
        pages=pages,
        page_rows=page_rows,
        page_size=page_size,
        n_groups=n_groups,
        per_group=per_group,
        list_rows=list_rows,
    )
    vmem = pl.BlockSpec(memory_space=pltpu.VMEM)
    smem = pl.BlockSpec(memory_space=pltpu.SMEM)
    hbm = pl.BlockSpec(memory_space=pl.ANY)
    dma = pltpu.SemaphoreType.DMA
    info = pl.pallas_call(
        functools.partial(list_kernel, cfg),
        out_shape=jax.ShapeDtypeStruct((sources, info_rows, LANES), I32),
        in_specs=[smem, vmem],
        out_specs=vmem,
        name="lists",
    )(lengths, page_table)
    return pl.pallas_call(
        functools.partial(kernel, cfg),
        out_shape=jax.ShapeDtypeStruct((requests, columns // nz), BF16),
        in_specs=[vmem, vmem, vmem, hbm, hbm, hbm, hbm],
        out_specs=vmem,
        scratch_shapes=[
            pltpu.VMEM(info.shape, I32),
            pltpu.VMEM((mark_rows, LANES), I32),
            pltpu.SMEM((mark_rows, LANES), I32),
            pltpu.VMEM((flat_rows, LANES), I32),
            pltpu.SMEM((flat_rows, LANES), I32),
            pltpu.VMEM((requests, heads, dim), BF16),
            pltpu.VMEM(k_rows.shape, BF16),
            pltpu.VMEM(v_rows.shape, BF16),
            pltpu.VMEM(out_weight.shape, BF16),
            pltpu.VMEM((pages, 1, LANES), F32),
            pltpu.VMEM((pages, 1, LANES), F32),
            pltpu.VMEM((n_groups, 1, LANES), F32),
            pltpu.VMEM((n_groups, heads, LANES), F32),
            pltpu.VMEM((n_groups, heads, LANES), F32),
            pltpu.VMEM((n_groups, heads, LANES), F32),
            pltpu.VMEM((n_groups, heads, LANES), F32),
            pltpu.VMEM((chips, rows_here, heads, dim), BF16),
            pltpu.VMEM((chips, heads, LANES), F32),
            pltpu.VMEM((chips, rows_here, heads, dim), BF16),
            pltpu.VMEM((chips, heads, LANES), F32),
            pltpu.VMEM((chips, rows_here, heads, dim), BF16),
            pltpu.VMEM((chips, heads, LANES), F32),
            pltpu.VMEM((chips, rows_here, heads, dim), BF16),
            pltpu.VMEM((chips, heads, LANES), F32),
            pltpu.VMEM((rows_here * heads, dim), F32),
            pltpu.VMEM((sources, rows_here, width), BF16),
            pltpu.VMEM((nz, requests, columns // nz), BF16),
            pltpu.VMEM((nz, requests, columns // nz), BF16),
            dma,
            dma((3, 4)),
            dma,
            dma,
            dma,
            dma((sources,)),
            dma((sources,)),
            dma((sources,)),
            dma((sources,)),
            dma((sources,)),
            dma((chips,)),
            dma((chips,)),
            dma((chips,)),
            dma((chips,)),
            dma((chips,)),
            dma((chips,)),
            dma((chips,)),
            dma((chips,)),
            dma((sources,)),
            dma((sources,)),
            dma((sources,)),
            dma((nz,)),
            dma((nz,)),
        ],
        compiler_params=pltpu.CompilerParams(
            vmem_limit_bytes=62 * 1024 * 1024, collective_id=0, has_side_effects=True
        ),
        name="paged",
    )(
        info,
        key_page_scale.T,
        value_page_scale.T,
        queries,
        k_rows,
        v_rows,
        out_weight,
    )


def solution(mesh):
    in_specs = (
        P("req", "head", None),
        P("req", None, "head", None),
        P("req", None, "head", None),
        P("req", "head"),
        P("req", "head"),
        P("req"),
        P("req", None),
        P("head", "req"),
    )
    out_specs = P(None, ("req", "head"))
    return jax.shard_map(
        on_device, mesh=mesh, in_specs=in_specs, out_specs=out_specs, check_vma=False
    )
```

```python
import functools
import math

import jax
import jax.numpy as jnp
from jax import lax
from jax.experimental import pallas as pl
from jax.experimental.pallas import tpu as pltpu
from jax.sharding import PartitionSpec as P

MESH = pl.DeviceIdType.MESH
FLOOR = -1e30
DROP = -3e38
LANES = 128
SUB = 8
LIVE_BITS = 5
OWNER_SHIFT = 7
FIELDS = 8
ROUND = LANES // FIELDS
F32 = jnp.float32
BF16 = jnp.bfloat16
I32 = jnp.int32


def nt(a, b):
    return lax.dot_general(a, b, (((1,), (1,)), ((), ())), preferred_element_type=F32)


def nn(a, b):
    return jnp.dot(a, b, preferred_element_type=F32)


def iota(shape, axis):
    return lax.broadcasted_iota(I32, shape, axis)


def list_kernel(cfg, lengths_ref, table_ref, out_ref):
    sources, rows_here, pages = cfg["sources"], cfg["rows_here"], cfg["pages"]
    page_size, per_group = cfg["page_size"], cfg["per_group"]
    list_rows = cfg["list_rows"]
    shape = (rows_here, LANES)
    row_id = iota(shape, 0)
    lengths = jnp.zeros(shape, I32)
    for r in range(rows_here):
        lengths = jnp.where(row_id == r, lengths_ref[r], lengths)
    live = jnp.minimum(lengths - iota(shape, 1) * page_size, page_size)
    table = table_ref[...]
    locals_, mines = [], []
    for d in range(sources):
        local = table - d * pages
        locals_.append(local)
        mines.append((live > 0) & (local >= 0) & (local < pages))
    flag = jnp.concatenate([jnp.where(m, 1.0, 0.0) for m in mines], axis=0).astype(BF16)
    total = sources * rows_here
    up = jnp.where(iota((LANES, LANES), 0) < iota((LANES, LANES), 1), 1.0, 0.0).astype(BF16)
    before = nn(flag, up)
    count = nn(flag, jnp.ones((LANES, LANES), BF16))
    need = jnp.floor((count + (per_group - 1)) * (1.0 / per_group))
    i, j = iota((total, total), 0), iota((total, total), 1)
    tri = jnp.where((i >= j) & (i // rows_here == j // rows_here), 1.0, 0.0).astype(BF16)
    ends = nn(tri, need.astype(BF16))
    starts = ends - need
    before, starts_int, need_int = before.astype(I32), starts.astype(I32), need.astype(I32)

    high = jnp.full(shape, -1, I32)
    low, lead, page, rest = high, high, high, high
    for d in range(sources):
        rows = slice(d * rows_here, (d + 1) * rows_here)
        step = before[rows] >> 2
        group = starts_int[rows] + step
        column = (group & (ROUND - 1)) * FIELDS
        place = before[rows] & 3
        high = jnp.where(mines[d], d * list_rows + group // ROUND, high)
        low = jnp.where(mines[d], column + place, low)
        lead = jnp.where(mines[d] & (place == 0), column + per_group, lead)
        page = jnp.where(mines[d], locals_[d], page)
        left = (need_int[rows] - 1 - step) * 2 + jnp.where(step == 0, 1, 0)
        rest = jnp.where(mines[d], left, rest)
    one = (page >> 2).astype(F32)
    two = ((page & 3) * (1 << LIVE_BITS) + live).astype(F32)
    rest = rest.astype(F32)
    hi_rows = -(-(sources * list_rows) // 16) * 16
    hi_iota, lo_iota = iota((hi_rows, LANES), 0), iota((LANES, LANES), 0)
    lefts, rights = [], []
    for r in range(rows_here):
        row = slice(r, r + 1)
        lefts.append(jnp.where(hi_iota == high[row], 1.0, 0.0).astype(BF16))
        same, head = lo_iota == low[row], lo_iota == lead[row]
        pair = [
            jnp.where(same, one[row], jnp.where(head, float(r), 0.0)),
            jnp.where(same, two[row], jnp.where(head, rest[row], 0.0)),
        ]
        rights.append(jnp.concatenate(pair, axis=0).astype(BF16))
    found = nt(jnp.concatenate(lefts, axis=1), jnp.concatenate(rights, axis=1))
    found = (found[:, :LANES] * float(4 << LIVE_BITS) + found[:, LANES:]).astype(I32)

    diag = row_id == iota(shape, 1)
    for d in range(sources):
        rows = slice(d * rows_here, (d + 1) * rows_here)
        end, some = ends[rows], need[rows] > 0.5
        out_ref[d, :list_rows, :] = found[d * list_rows : (d + 1) * list_rows]
        mark = jnp.maximum(end - 1.0, 0.0) * 2.0 + jnp.where(some, 1.0, 0.0)
        mark = jnp.sum(jnp.where(diag, mark, 0.0), axis=0, keepdims=True)
        size = jnp.max(end, axis=0, keepdims=True)
        mark = jnp.where(iota((1, LANES), 1) == rows_here, size, mark)
        out_ref[d, list_rows : list_rows + 1, :] = mark.astype(I32)


def kernel(
    cfg,
    info_hbm,
    kscale_hbm,
    vscale_hbm,
    q_hbm,
    k_hbm,
    v_hbm,
    w_hbm,
    out_ref,
    info_ref,
    kscale_ref,
    vscale_ref,
    info_all,
    mark_vmem,
    marks,
    flat_vmem,
    flat,
    q_all,
    k_buf,
    v_buf,
    w_buf,
    kse,
    vse,
    bias,
    scores,
    peaks,
    dens,
    accs,
    pair_send,
    pair_lse_send,
    pair_recv,
    pair_lse_recv,
    num_send,
    lse_send,
    num_recv,
    lse_recv,
    mixed,
    att_all,
    term_send,
    term_recv,
    own_terms,
    q_sem,
    load_sems,
    info_sem,
    small_sems,
    mark_sem,
    flat_sem,
    t_send,
    t_recv,
    q_send,
    q_recv,
    q_pass,
    p_send,
    p_recv,
    pl_send,
    pl_recv,
    n_send,
    n_recv,
    l_send,
    l_recv,
    a_send,
    a_recv,
    a_pass,
    z_send,
    z_recv,
):
    sources, nz = cfg["sources"], cfg["nz"]
    rows_here, heads, dim = cfg["rows_here"], cfg["heads"], cfg["dim"]
    pages, page_rows, page_size = cfg["pages"], cfg["page_rows"], cfg["page_size"]
    requests = rows_here * sources
    kv_local = page_rows // page_size
    per_group = LANES // page_rows
    n_groups = cfg["n_groups"]
    steps = n_groups // ROUND
    width = heads * dim
    me = lax.axis_index("req")
    mz = lax.axis_index("head")
    chips = sources // 2
    chip, core = me // 2, lax.rem(me, 2)
    partner = me + 1 - 2 * core

    def other_chip(k):
        return lax.rem(chip + k, chips)

    far = range(chips - 1, 0, -1)
    list_rows = cfg["list_rows"]
    flat_rows = flat_vmem.shape[0]

    barrier = pltpu.get_barrier_semaphore()
    for k in range(1, sources):
        pl.semaphore_signal(
            barrier, inc=1, device_id={"req": lax.rem(me + k, sources)}, device_id_type=MESH
        )
    for k in range(1, nz):
        pl.semaphore_signal(barrier, inc=1, device_id={"head": lax.rem(mz + k, nz)}, device_id_type=MESH)
    q_load = pltpu.make_async_copy(q_hbm, q_all.at[pl.ds(me * rows_here, rows_here)], q_sem)
    q_load.start()
    info_load = pltpu.make_async_copy(info_hbm.at[me], info_all.at[me], info_sem)
    info_load.start()
    smalls = []
    pairs = ((info_hbm, info_ref), (kscale_hbm, kscale_ref), (vscale_hbm, vscale_ref))
    for n, (src, dst) in enumerate(pairs):
        cp = pltpu.make_async_copy(src, dst, small_sems.at[n])
        cp.start()
        smalls.append(cp)
    loads = []
    parts = load_sems.shape[1]
    for which, (src, dst) in enumerate(((k_hbm, k_buf), (v_hbm, v_buf), (w_hbm, w_buf))):
        chunk = src.shape[0] // parts
        for c in range(parts):
            rows = pl.ds(c * chunk, chunk)
            cp = pltpu.make_async_copy(src.at[rows], dst.at[rows], load_sems.at[which, c])
            cp.start()
            loads.append(cp)
    k_loads, v_loads, w_loads = loads[:parts], loads[parts : 2 * parts], loads[2 * parts :]

    pl.semaphore_wait(barrier, sources + nz - 2)

    def info_copy(peer, owner):
        return pltpu.make_async_remote_copy(
            src_ref=info_ref.at[peer],
            dst_ref=info_all.at[owner],
            send_sem=t_send.at[peer],
            recv_sem=t_recv.at[owner],
            device_id={"req": peer},
            device_id_type=MESH,
        )

    def remote(src, dst, send, recv, **where):
        return pltpu.make_async_remote_copy(
            src_ref=src,
            dst_ref=dst,
            send_sem=send,
            recv_sem=recv,
            device_id=where,
            device_id_type=MESH,
        )

    def gather(rows_of, send, recv, passing):
        def direct(peer, owner):
            return remote(rows_of(owner), rows_of(owner), send.at[peer], recv.at[owner], req=peer)

        def onward(owner):
            return remote(rows_of(owner), rows_of(owner), passing.at[owner], recv.at[owner], req=partner)

        def begin():
            for k in far:
                direct(other_chip(k) * 2 + core, me).start()
            direct(partner, me).start()

        def pass_on(k):
            owner = other_chip(k) * 2 + core
            direct(owner, owner).wait_recv()
            onward(owner).start()

        def take(k):
            owner = other_chip(k) * 2 + 1 - core
            if k == 0:
                direct(partner, partner).wait_recv()
            else:
                onward(owner).wait_recv()

        def finish():
            direct(partner, me).wait_send()
            for k in far:
                owner = other_chip(k) * 2 + core
                direct(owner, me).wait_send()
                onward(owner).wait_send()

        return begin, pass_on, take, finish

    q_begin, q_pass_on, q_take, q_finish = gather(
        lambda owner: q_all.at[pl.ds(owner * rows_here, rows_here)], q_send, q_recv, q_pass
    )
    smalls[0].wait()
    for k in range(sources - 1, 0, -1):
        info_copy(lax.rem(me + k, sources), me).start()
    q_load.wait()
    q_begin()

    for cp in smalls[1:]:
        cp.wait()
    lane_sub = iota((LANES, LANES), 0)
    for src, dst, factor in ((kscale_ref, kse, 1.0 / math.sqrt(dim)), (vscale_ref, vse, 1.0)):
        for b in range(pages // LANES):
            cols = slice(b * LANES, (b + 1) * LANES)
            both = src[kv_local - 1 : kv_local, cols]
            for v in range(kv_local - 1):
                both = jnp.where(lane_sub % kv_local == v, src[v : v + 1, cols], both)
            both = jnp.broadcast_to(both * factor, (LANES, LANES)).T
            dst[b * LANES : (b + 1) * LANES, 0, :] = both

    info_load.wait()
    for k in range(1, sources):
        peer = lax.rem(me + k, sources)
        info_copy(peer, peer).wait_recv()
    for src in range(sources):
        mark_vmem[src : src + 1, :] = info_all[src, list_rows : list_rows + 1, :]
    to_smem = pltpu.make_async_copy(mark_vmem, marks, mark_sem)
    to_smem.start()
    to_smem.wait()

    shape = (flat_rows, LANES)
    lane, field = iota(shape, 1), iota(shape, 1) % FIELDS
    group = iota(shape, 0) * ROUND + lane // FIELDS
    joined = jnp.zeros(shape, I32)
    base = jnp.int32(0)
    for src in range(sources):
        size = marks[src, rows_here]
        rows = min(flat_rows, info_all.shape[1])
        one = info_all[src, :rows, :]
        if rows < flat_rows:
            one = jnp.concatenate([one, jnp.zeros((flat_rows - rows, LANES), I32)], axis=0)
        one = jnp.where(field == per_group, one + (src * rows_here << OWNER_SHIFT), one)
        move = (base & (ROUND - 1)) * FIELDS
        one = pltpu.roll(one, move, axis=1)
        one = jnp.where(lane < move, pltpu.roll(one, 1, axis=0), one)
        one = pltpu.roll(one, base // ROUND, axis=0)
        joined = jnp.where((group >= base) & (group < base + size), one, joined)
        base = base + size
    low_bits = (1 << OWNER_SHIFT) - 1
    last = group + ((pltpu.roll(joined, 1, axis=1) & low_bits) >> 1)
    fresh = pltpu.roll(joined, 2, axis=1) & 1
    values = jnp.where(field == per_group + 1, last, fresh)
    values = jnp.where(field == per_group, joined >> OWNER_SHIFT, values)
    flat_vmem[...] = jnp.where(field < per_group, joined >> LIVE_BITS, values)
    to_smem = pltpu.make_async_copy(flat_vmem, flat, flat_sem)
    to_smem.start()

    live = jnp.where(field < per_group, joined & ((1 << LIVE_BITS) - 1), 0).astype(F32)
    spread = iota((LANES, LANES), 0) % FIELDS == iota((LANES, LANES), 1) // page_rows
    spread = jnp.where(spread, 1.0, 0.0).astype(BF16)
    chosen = iota((ROUND, LANES), 1) // FIELDS == iota((ROUND, LANES), 0)
    token_row = ((iota((1, LANES), 1) % page_rows) // kv_local).astype(F32)
    picks = [jnp.where(chosen, live[b : b + 1], 0.0) for b in range(steps)]
    wide = nn(jnp.concatenate(picks, axis=0).astype(BF16), spread)
    bias[:, 0, :] = jnp.where(token_row < wide, 0.0, FLOOR)
    to_smem.wait()

    for k in far:
        q_pass_on(k)
    for k in range(chips):
        q_take(k)
    for cp in k_loads:
        cp.wait()

    lane8 = iota((SUB, LANES), 1)
    token = (lane8 % page_rows) // kv_local
    per_head = heads // kv_local
    kv_masks = [lane8 % kv_local == (t * SUB) // per_head for t in range(heads // SUB)]
    blank = jnp.zeros((heads, dim), BF16)

    def by_page(parts):
        got = parts[per_group - 1]
        for i in range(per_group - 2, -1, -1):
            got = jnp.where(lane8 < (i + 1) * page_rows, parts[i], got)
        return got

    def fetch(ref, page_ids):
        return jnp.concatenate([ref[p] for p in page_ids], axis=0)

    def scale_row(ref, page_ids):
        return by_page([jnp.broadcast_to(ref[p], (SUB, LANES)) for p in page_ids])

    def same_owner(it, j):
        return jnp.full((heads, LANES), flat[it, j * FIELDS + per_group + 2], I32) == 0

    def score_step(it, top):
        for pair in range(ROUND // 2):
            js = (2 * pair, 2 * pair + 1)
            ids = [[flat[it, j * FIELDS + i] for i in range(per_group)] for j in js]
            kk = jnp.concatenate([fetch(k_buf, one) for one in ids], axis=1)
            qa, qb = [q_all[flat[it, j * FIELDS + per_group]] for j in js]
            lhs = jnp.concatenate(
                [jnp.concatenate([qa, blank], axis=1), jnp.concatenate([blank, qb], axis=1)], axis=0
            )
            s = nt(lhs, kk)
            for x, j in enumerate(js):
                g = it * ROUND + j
                scale = scale_row(kse, ids[x])
                shift = jnp.broadcast_to(bias[g], (SUB, LANES))
                tiles = []
                for t in range(heads // SUB):
                    tile = s[x * heads + t * SUB : x * heads + (t + 1) * SUB] * scale + shift
                    tiles.append(jnp.where(kv_masks[t], tile, FLOOR))
                tile = jnp.concatenate(tiles, axis=0)
                scores[g] = tile
                mine = jnp.broadcast_to(jnp.max(tile, axis=1, keepdims=True), (heads, LANES))
                top = jnp.where(same_owner(it, j), jnp.maximum(top, mine), mine)
                peaks[g] = top
        return top

    lax.fori_loop(0, steps, score_step, jnp.full((heads, LANES), FLOOR, F32))
    for cp in v_loads:
        cp.wait()

    def value_step(it, carry):
        acc, den = carry
        for pair in range(ROUND // 2):
            js = (2 * pair, 2 * pair + 1)
            ids = [[flat[it, j * FIELDS + i] for i in range(per_group)] for j in js]
            vv = jnp.concatenate([fetch(v_buf, one) for one in ids], axis=1)
            lhs, weights = [], []
            for x, j in enumerate(js):
                weight = jnp.exp(scores[it * ROUND + j] - peaks[flat[it, j * FIELDS + per_group + 1]])
                scale = scale_row(vse, ids[x])
                scaled = [weight[t * SUB : (t + 1) * SUB] * scale for t in range(heads // SUB)]
                lhs.append(jnp.concatenate(scaled, axis=0).astype(BF16))
                weights.append(weight)
            o = nn(jnp.concatenate(lhs, axis=0), vv)
            for x, j in enumerate(js):
                g = it * ROUND + j
                keep = same_owner(it, j)
                mine = o[x * heads : (x + 1) * heads, x * dim : (x + 1) * dim]
                acc = jnp.where(keep, acc + mine, mine)
                den = jnp.where(keep, den + weights[x], weights[x])
                accs[g] = acc
                dens[g] = den
        return acc, den

    zero = jnp.zeros((heads, LANES), F32)
    lax.fori_loop(0, steps, value_step, (zero, zero))

    lane16 = iota((heads, LANES), 1)

    def first_group(dest):
        base = jnp.int32(0)
        for src in range(sources):
            base = base + jnp.where(src < dest, marks[src, rows_here], 0)
        return base

    def local_part(dest, base, r):
        mark = marks[dest, r]
        last = base + (mark >> 1)
        some = (mark & 1).astype(F32)
        den = jnp.broadcast_to(jnp.sum(dens[last], axis=1, keepdims=True), (heads, LANES))
        den = jnp.maximum(den, 0.5)
        num = accs[last] * (some / den)
        return num, (peaks[last] + jnp.log(den)) * some + (some - 1.0) * (-FLOOR)

    def pair_copy(c):
        return remote(pair_send.at[c], pair_recv.at[c], p_send.at[c], p_recv.at[c], req=partner)

    def pair_lse_copy(c):
        return remote(pair_lse_send.at[c], pair_lse_recv.at[c], pl_send.at[c], pl_recv.at[c], req=partner)

    def num_copy(to, owner):
        return remote(
            num_send.at[to], num_recv.at[owner], n_send.at[to], n_recv.at[owner], req=to * 2 + core
        )

    def lse_copy(to, owner):
        return remote(
            lse_send.at[to], lse_recv.at[owner], l_send.at[to], l_recv.at[owner], req=to * 2 + core
        )

    def for_partner(k, carry):
        c = other_chip(chips - 1 - k)
        dest = c * 2 + 1 - core
        base = first_group(dest)
        tile = jnp.full((heads, LANES), FLOOR, F32)
        for r in range(rows_here):
            num, lse = local_part(dest, base, r)
            pair_send[c, r] = num.astype(BF16)
            tile = jnp.where(lane16 == r, lse, tile)
        pair_lse_send[c] = tile
        pair_copy(c).start()
        pair_lse_copy(c).start()
        return carry

    lax.fori_loop(0, chips, for_partner, 0)

    def merge(c, num_at, lse_at):
        dest = c * 2 + core
        base = first_group(dest)
        theirs = pair_lse_recv[c]
        tile = jnp.full((heads, LANES), FLOOR, F32)
        for r in range(rows_here):
            num, lse = local_part(dest, base, r)
            their = jnp.broadcast_to(theirs[:, r : r + 1], (heads, LANES))
            high = jnp.maximum(lse, their)
            a, b = jnp.exp(lse - high), jnp.exp(their - high)
            total = a + b
            got = (num * a + pair_recv[c, r].astype(F32) * b) / total
            num_at[r] = got.astype(BF16)
            tile = jnp.where(lane16 == r, high + jnp.log(total), tile)
        lse_at[...] = tile

    def send_block(k, carry):
        c = other_chip(chips - 1 - k)
        merge(c, num_send.at[c], lse_send.at[c])
        num_copy(c, chip).start()
        lse_copy(c, chip).start()
        return carry

    for k in range(chips - 1, -1, -1):
        pair_lse_copy(other_chip(k)).wait_recv()
        pair_copy(other_chip(k)).wait_recv()
    lax.fori_loop(0, chips - 1, send_block, 0)
    merge(chip, num_recv.at[chip], lse_recv.at[chip])
    for k in far:
        c = other_chip(k)
        lse_copy(c, c).wait_recv()
        num_copy(c, c).wait_recv()

    lses = [lse_recv[s] for s in range(chips)]
    top = functools.reduce(jnp.maximum, lses)
    shares = [jnp.exp(x - top) for x in lses]
    total = functools.reduce(jnp.add, shares)
    shares = [x / total for x in shares]
    for r in range(rows_here):
        got = jnp.zeros((heads, dim), F32)
        for s in range(chips):
            share = jnp.broadcast_to(shares[s][:, r : r + 1], (heads, dim))
            got = got + share * num_recv[s, r].astype(F32)
        mixed[r * heads : (r + 1) * heads, :] = got
    for h in range(heads):
        rows = mixed[pl.ds(h, rows_here, stride=heads), :]
        att_all[me, :, h * dim : (h + 1) * dim] = rows.astype(BF16)

    a_begin, a_pass_on, a_take, a_finish = gather(lambda owner: att_all.at[owner], a_send, a_recv, a_pass)
    a_begin()
    for cp in w_loads:
        cp.wait()

    cols = w_buf.shape[1] // nz
    block_rows = 2 * rows_here

    def term_copy(to, owner, c):
        return remote(
            term_send.at[to, c], term_recv.at[owner, c], z_send.at[to, c], z_recv.at[owner, c], head=to
        )

    def project(c):
        att = att_all[pl.ds(2 * c, 2)].reshape(block_rows, width)
        if cols % LANES == 0:
            for k in range(1, nz):
                peer = lax.rem(mz + k, nz)
                columns = pl.ds(pl.multiple_of(peer * cols, cols), cols)
                term_send[peer, c] = nn(att, w_buf[:, columns]).astype(BF16)
                term_copy(peer, mz, c).start()
            own_terms[c] = nn(att, w_buf[:, pl.ds(pl.multiple_of(mz * cols, cols), cols)])
        else:
            every = nn(att, w_buf[...])
            for z in range(nz):
                term_send[z, c] = every[:, z * cols : (z + 1) * cols].astype(BF16)
            for k in range(1, nz):
                term_copy(lax.rem(mz + k, nz), mz, c).start()
            own_terms[c] = term_send[mz, c].astype(F32)

    order = sorted(range(1, chips), key=lambda k: (k % 2, k))
    a_take(0)
    ready = 0
    for k in order:
        a_pass_on(k)
        project(other_chip(ready))
        a_take(k)
        ready = k
    project(other_chip(ready))
    for k in [0] + order:
        c = other_chip(k)
        got = own_terms[c]
        for z in range(1, nz):
            peer = lax.rem(mz + z, nz)
            term_copy(peer, peer, c).wait_recv()
            got = got + term_recv[peer, c].astype(F32)
        out_ref[pl.ds(pl.multiple_of(c * block_rows, block_rows), block_rows), :] = got.astype(BF16)

    for k in range(1, sources):
        peer = lax.rem(me + k, sources)
        info_copy(peer, me).wait_send()
    q_finish()
    a_finish()
    for c in range(chips):
        pair_copy(c).wait_send()
        pair_lse_copy(c).wait_send()
    for k in far:
        c = other_chip(k)
        num_copy(c, chip).wait_send()
        lse_copy(c, chip).wait_send()
    for k in range(1, nz):
        for c in range(chips):
            term_copy(lax.rem(mz + k, nz), mz, c).wait_send()


def on_device(
    queries,
    k_codes,
    value_quantized_codes,
    key_page_scale,
    value_page_scale,
    lengths,
    page_table,
    out_weight,
):
    pages, page_size, kv_local, dim = k_codes.shape
    rows_here, heads, _ = queries.shape
    sources, nz = lax.axis_size("req"), lax.axis_size("head")
    requests = rows_here * sources
    page_rows = page_size * kv_local
    per_group = LANES // page_rows
    group_bound = (pages + (per_group - 1) * requests) // per_group
    n_groups = -(-group_bound // ROUND) * ROUND
    list_bound = (pages + (per_group - 1) * rows_here) // per_group
    list_rows = -(-list_bound // ROUND)
    info_rows = -(-(list_rows + 1) // SUB) * SUB
    flat_rows = -(-(n_groups // ROUND) // SUB) * SUB
    mark_rows = -(-sources // SUB) * SUB
    chips = sources // 2
    k_rows = k_codes.reshape(pages, page_rows, dim)
    v_rows = value_quantized_codes.reshape(pages, page_rows, dim)
    width = heads * dim
    columns = out_weight.shape[1]
    cfg = dict(
        sources=sources,
        nz=nz,
        rows_here=rows_here,
        heads=heads,
        dim=dim,
        pages=pages,
        page_rows=page_rows,
        page_size=page_size,
        n_groups=n_groups,
        per_group=per_group,
        list_rows=list_rows,
    )
    vmem = pl.BlockSpec(memory_space=pltpu.VMEM)
    smem = pl.BlockSpec(memory_space=pltpu.SMEM)
    hbm = pl.BlockSpec(memory_space=pl.ANY)
    dma = pltpu.SemaphoreType.DMA
    info = pl.pallas_call(
        functools.partial(list_kernel, cfg),
        out_shape=jax.ShapeDtypeStruct((sources, info_rows, LANES), I32),
        in_specs=[smem, vmem],
        out_specs=vmem,
        name="lists",
    )(lengths, page_table)
    return pl.pallas_call(
        functools.partial(kernel, cfg),
        out_shape=jax.ShapeDtypeStruct((requests, columns // nz), BF16),
        in_specs=[hbm] * 7,
        out_specs=vmem,
        scratch_shapes=[
            pltpu.VMEM(info.shape, I32),
            pltpu.VMEM((kv_local, pages), F32),
            pltpu.VMEM((kv_local, pages), F32),
            pltpu.VMEM(info.shape, I32),
            pltpu.VMEM((mark_rows, LANES), I32),
            pltpu.SMEM((mark_rows, LANES), I32),
            pltpu.VMEM((flat_rows, LANES), I32),
            pltpu.SMEM((flat_rows, LANES), I32),
            pltpu.VMEM((requests, heads, dim), BF16),
            pltpu.VMEM(k_rows.shape, BF16),
            pltpu.VMEM(v_rows.shape, BF16),
            pltpu.VMEM(out_weight.shape, BF16),
            pltpu.VMEM((pages, 1, LANES), F32),
            pltpu.VMEM((pages, 1, LANES), F32),
            pltpu.VMEM((n_groups, 1, LANES), F32),
            pltpu.VMEM((n_groups, heads, LANES), F32),
            pltpu.VMEM((n_groups, heads, LANES), F32),
            pltpu.VMEM((n_groups, heads, LANES), F32),
            pltpu.VMEM((n_groups, heads, LANES), F32),
            pltpu.VMEM((chips, rows_here, heads, dim), BF16),
            pltpu.VMEM((chips, heads, LANES), F32),
            pltpu.VMEM((chips, rows_here, heads, dim), BF16),
            pltpu.VMEM((chips, heads, LANES), F32),
            pltpu.VMEM((chips, rows_here, heads, dim), BF16),
            pltpu.VMEM((chips, heads, LANES), F32),
            pltpu.VMEM((chips, rows_here, heads, dim), BF16),
            pltpu.VMEM((chips, heads, LANES), F32),
            pltpu.VMEM((rows_here * heads, dim), F32),
            pltpu.VMEM((sources, rows_here, width), BF16),
            pltpu.VMEM((nz, chips, 2 * rows_here, columns // nz), BF16),
            pltpu.VMEM((nz, chips, 2 * rows_here, columns // nz), BF16),
            pltpu.VMEM((chips, 2 * rows_here, columns // nz), F32),
            dma,
            dma((3, 4)),
            dma,
            dma((3,)),
            dma,
            dma,
            dma((sources,)),
            dma((sources,)),
            dma((sources,)),
            dma((sources,)),
            dma((sources,)),
            dma((chips,)),
            dma((chips,)),
            dma((chips,)),
            dma((chips,)),
            dma((chips,)),
            dma((chips,)),
            dma((chips,)),
            dma((chips,)),
            dma((sources,)),
            dma((sources,)),
            dma((sources,)),
            dma((nz, chips)),
            dma((nz, chips)),
        ],
        compiler_params=pltpu.CompilerParams(
            vmem_limit_bytes=62 * 1024 * 1024, collective_id=0, has_side_effects=True
        ),
        name="paged",
    )(
        info,
        key_page_scale.T,
        value_page_scale.T,
        queries,
        k_rows,
        v_rows,
        out_weight,
    )


def solution(mesh):
    in_specs = (
        P("req", "head", None),
        P("req", None, "head", None),
        P("req", None, "head", None),
        P("req", "head"),
        P("req", "head"),
        P("req"),
        P("req", None),
        P("head", "req"),
    )
    out_specs = P(None, ("req", "head"))
    return jax.shard_map(
        on_device, mesh=mesh, in_specs=in_specs, out_specs=out_specs, check_vma=False
    )
```

```python
import functools
import math

import jax
import jax.numpy as jnp
from jax import lax
from jax.experimental import pallas as pl
from jax.experimental.pallas import tpu as pltpu
from jax.sharding import PartitionSpec as P

MESH = pl.DeviceIdType.MESH
FLOOR = -1e30
DROP = -3e38
LANES = 128
SUB = 8
LIVE_BITS = 5
OWNER_SHIFT = 7
FIELDS = 8
ROUND = LANES // FIELDS
F32 = jnp.float32
BF16 = jnp.bfloat16
I32 = jnp.int32


def nt(a, b):
    return lax.dot_general(a, b, (((1,), (1,)), ((), ())), preferred_element_type=F32)


def nn(a, b):
    return jnp.dot(a, b, preferred_element_type=F32)


def iota(shape, axis):
    return lax.broadcasted_iota(I32, shape, axis)


def list_kernel(cfg, lengths_ref, table_ref, out_ref):
    sources, rows_here, pages = cfg["sources"], cfg["rows_here"], cfg["pages"]
    page_size, per_group = cfg["page_size"], cfg["per_group"]
    list_rows = cfg["list_rows"]
    shape = (rows_here, LANES)
    row_id = iota(shape, 0)
    lengths = jnp.zeros(shape, I32)
    for r in range(rows_here):
        lengths = jnp.where(row_id == r, lengths_ref[r], lengths)
    live = jnp.minimum(lengths - iota(shape, 1) * page_size, page_size)
    table = table_ref[...]
    locals_, mines = [], []
    for d in range(sources):
        local = table - d * pages
        locals_.append(local)
        mines.append((live > 0) & (local >= 0) & (local < pages))
    flag = jnp.concatenate([jnp.where(m, 1.0, 0.0) for m in mines], axis=0).astype(BF16)
    total = sources * rows_here
    up = jnp.where(iota((LANES, LANES), 0) < iota((LANES, LANES), 1), 1.0, 0.0).astype(BF16)
    before = nn(flag, up)
    count = nn(flag, jnp.ones((LANES, LANES), BF16))
    need = jnp.floor((count + (per_group - 1)) * (1.0 / per_group))
    i, j = iota((total, total), 0), iota((total, total), 1)
    tri = jnp.where((i >= j) & (i // rows_here == j // rows_here), 1.0, 0.0).astype(BF16)
    ends = nn(tri, need.astype(BF16))
    starts = ends - need
    before, starts_int, need_int = before.astype(I32), starts.astype(I32), need.astype(I32)

    high = jnp.full(shape, -1, I32)
    low, lead, page, rest = high, high, high, high
    for d in range(sources):
        rows = slice(d * rows_here, (d + 1) * rows_here)
        step = before[rows] >> 2
        group = starts_int[rows] + step
        column = (group & (ROUND - 1)) * FIELDS
        place = before[rows] & 3
        high = jnp.where(mines[d], d * list_rows + group // ROUND, high)
        low = jnp.where(mines[d], column + place, low)
        lead = jnp.where(mines[d] & (place == 0), column + per_group, lead)
        page = jnp.where(mines[d], locals_[d], page)
        left = (need_int[rows] - 1 - step) * 2 + jnp.where(step == 0, 1, 0)
        rest = jnp.where(mines[d], left, rest)
    one = (page >> 2).astype(F32)
    two = ((page & 3) * (1 << LIVE_BITS) + live).astype(F32)
    rest = rest.astype(F32)
    hi_rows = -(-(sources * list_rows) // 16) * 16
    hi_iota, lo_iota = iota((hi_rows, LANES), 0), iota((LANES, LANES), 0)
    lefts, rights = [], []
    for r in range(rows_here):
        row = slice(r, r + 1)
        lefts.append(jnp.where(hi_iota == high[row], 1.0, 0.0).astype(BF16))
        same, head = lo_iota == low[row], lo_iota == lead[row]
        pair = [
            jnp.where(same, one[row], jnp.where(head, float(r), 0.0)),
            jnp.where(same, two[row], jnp.where(head, rest[row], 0.0)),
        ]
        rights.append(jnp.concatenate(pair, axis=0).astype(BF16))
    found = nt(jnp.concatenate(lefts, axis=1), jnp.concatenate(rights, axis=1))
    found = (found[:, :LANES] * float(4 << LIVE_BITS) + found[:, LANES:]).astype(I32)

    diag = row_id == iota(shape, 1)
    for d in range(sources):
        rows = slice(d * rows_here, (d + 1) * rows_here)
        end, some = ends[rows], need[rows] > 0.5
        out_ref[d, :list_rows, :] = found[d * list_rows : (d + 1) * list_rows]
        mark = jnp.maximum(end - 1.0, 0.0) * 2.0 + jnp.where(some, 1.0, 0.0)
        mark = jnp.sum(jnp.where(diag, mark, 0.0), axis=0, keepdims=True)
        size = jnp.max(end, axis=0, keepdims=True)
        mark = jnp.where(iota((1, LANES), 1) == rows_here, size, mark)
        out_ref[d, list_rows : list_rows + 1, :] = mark.astype(I32)


def kernel(
    cfg,
    info_hbm,
    kscale_hbm,
    vscale_hbm,
    q_hbm,
    k_hbm,
    v_hbm,
    w_hbm,
    out_ref,
    info_ref,
    kscale_ref,
    vscale_ref,
    info_all,
    mark_vmem,
    marks,
    flat_vmem,
    flat,
    q_all,
    k_buf,
    v_buf,
    w_buf,
    kse,
    vse,
    bias,
    scores,
    peaks,
    dens,
    accs,
    pair_send,
    pair_lse_send,
    pair_recv,
    pair_lse_recv,
    num_send,
    lse_send,
    num_recv,
    lse_recv,
    mixed,
    att_all,
    term_send,
    term_recv,
    own_terms,
    q_sem,
    load_sems,
    info_sem,
    small_sems,
    mark_sem,
    flat_sem,
    t_send,
    t_recv,
    q_send,
    q_recv,
    q_pass,
    p_send,
    p_recv,
    pl_send,
    pl_recv,
    n_send,
    n_recv,
    l_send,
    l_recv,
    a_send,
    a_recv,
    a_pass,
    z_send,
    z_recv,
):
    sources, nz = cfg["sources"], cfg["nz"]
    rows_here, heads, dim = cfg["rows_here"], cfg["heads"], cfg["dim"]
    pages, page_rows, page_size = cfg["pages"], cfg["page_rows"], cfg["page_size"]
    requests = rows_here * sources
    kv_local = page_rows // page_size
    per_group = LANES // page_rows
    n_groups = cfg["n_groups"]
    steps = n_groups // ROUND
    width = heads * dim
    me = lax.axis_index("req")
    mz = lax.axis_index("head")
    chips = sources // 2
    chip, core = me // 2, lax.rem(me, 2)
    partner = me + 1 - 2 * core

    def other_chip(k):
        return lax.rem(chip + k, chips)

    far = range(chips - 1, 0, -1)
    list_rows = cfg["list_rows"]
    flat_rows = flat_vmem.shape[0]

    barrier = pltpu.get_barrier_semaphore()
    for k in range(1, sources):
        pl.semaphore_signal(
            barrier, inc=1, device_id={"req": lax.rem(me + k, sources)}, device_id_type=MESH
        )
    for k in range(1, nz):
        pl.semaphore_signal(barrier, inc=1, device_id={"head": lax.rem(mz + k, nz)}, device_id_type=MESH)
    q_load = pltpu.make_async_copy(q_hbm, q_all.at[pl.ds(me * rows_here, rows_here)], q_sem)
    q_load.start()
    info_load = pltpu.make_async_copy(info_hbm.at[me], info_all.at[me], info_sem)
    info_load.start()
    smalls = []
    pairs = ((info_hbm, info_ref), (kscale_hbm, kscale_ref), (vscale_hbm, vscale_ref))
    for n, (src, dst) in enumerate(pairs):
        cp = pltpu.make_async_copy(src, dst, small_sems.at[n])
        cp.start()
        smalls.append(cp)

    pl.semaphore_wait(barrier, sources + nz - 2)

    def info_copy(peer, owner):
        return pltpu.make_async_remote_copy(
            src_ref=info_ref.at[peer],
            dst_ref=info_all.at[owner],
            send_sem=t_send.at[peer],
            recv_sem=t_recv.at[owner],
            device_id={"req": peer},
            device_id_type=MESH,
        )

    def remote(src, dst, send, recv, **where):
        return pltpu.make_async_remote_copy(
            src_ref=src,
            dst_ref=dst,
            send_sem=send,
            recv_sem=recv,
            device_id=where,
            device_id_type=MESH,
        )

    def gather(rows_of, send, recv, passing):
        def direct(peer, owner):
            return remote(rows_of(owner), rows_of(owner), send.at[peer], recv.at[owner], req=peer)

        def onward(owner):
            return remote(rows_of(owner), rows_of(owner), passing.at[owner], recv.at[owner], req=partner)

        def begin():
            for k in far:
                direct(other_chip(k) * 2 + core, me).start()
            direct(partner, me).start()

        def pass_on(k):
            owner = other_chip(k) * 2 + core
            direct(owner, owner).wait_recv()
            onward(owner).start()

        def take(k):
            owner = other_chip(k) * 2 + 1 - core
            if k == 0:
                direct(partner, partner).wait_recv()
            else:
                onward(owner).wait_recv()

        def finish():
            direct(partner, me).wait_send()
            for k in far:
                owner = other_chip(k) * 2 + core
                direct(owner, me).wait_send()
                onward(owner).wait_send()

        return begin, pass_on, take, finish

    q_begin, q_pass_on, q_take, q_finish = gather(
        lambda owner: q_all.at[pl.ds(owner * rows_here, rows_here)], q_send, q_recv, q_pass
    )
    smalls[0].wait()
    for k in range(sources - 1, 0, -1):
        info_copy(lax.rem(me + k, sources), me).start()
    q_load.wait()
    for cp in smalls[1:]:
        cp.wait()
    q_begin()
    loads = []
    parts = load_sems.shape[1]
    for which, (src, dst) in enumerate(((k_hbm, k_buf), (v_hbm, v_buf), (w_hbm, w_buf))):
        chunk = src.shape[0] // parts
        for c in range(parts):
            rows = pl.ds(c * chunk, chunk)
            cp = pltpu.make_async_copy(src.at[rows], dst.at[rows], load_sems.at[which, c])
            cp.start()
            loads.append(cp)
    k_loads, v_loads, w_loads = loads[:parts], loads[parts : 2 * parts], loads[2 * parts :]

    lane_sub = iota((LANES, LANES), 0)
    for src, dst, factor in ((kscale_ref, kse, 1.0 / math.sqrt(dim)), (vscale_ref, vse, 1.0)):
        for b in range(pages // LANES):
            cols = slice(b * LANES, (b + 1) * LANES)
            both = src[kv_local - 1 : kv_local, cols]
            for v in range(kv_local - 1):
                both = jnp.where(lane_sub % kv_local == v, src[v : v + 1, cols], both)
            both = jnp.broadcast_to(both * factor, (LANES, LANES)).T
            dst[b * LANES : (b + 1) * LANES, 0, :] = both

    info_load.wait()
    for k in range(1, sources):
        peer = lax.rem(me + k, sources)
        info_copy(peer, peer).wait_recv()
    for src in range(sources):
        mark_vmem[src : src + 1, :] = info_all[src, list_rows : list_rows + 1, :]
    to_smem = pltpu.make_async_copy(mark_vmem, marks, mark_sem)
    to_smem.start()
    to_smem.wait()

    shape = (flat_rows, LANES)
    lane, field = iota(shape, 1), iota(shape, 1) % FIELDS
    group = iota(shape, 0) * ROUND + lane // FIELDS
    joined = jnp.zeros(shape, I32)
    base = jnp.int32(0)
    for src in range(sources):
        size = marks[src, rows_here]
        rows = min(flat_rows, info_all.shape[1])
        one = info_all[src, :rows, :]
        if rows < flat_rows:
            one = jnp.concatenate([one, jnp.zeros((flat_rows - rows, LANES), I32)], axis=0)
        one = jnp.where(field == per_group, one + (src * rows_here << OWNER_SHIFT), one)
        move = (base & (ROUND - 1)) * FIELDS
        one = pltpu.roll(one, move, axis=1)
        one = jnp.where(lane < move, pltpu.roll(one, 1, axis=0), one)
        one = pltpu.roll(one, base // ROUND, axis=0)
        joined = jnp.where((group >= base) & (group < base + size), one, joined)
        base = base + size
    low_bits = (1 << OWNER_SHIFT) - 1
    last = group + ((pltpu.roll(joined, 1, axis=1) & low_bits) >> 1)
    fresh = pltpu.roll(joined, 2, axis=1) & 1
    values = jnp.where(field == per_group + 1, last, fresh)
    values = jnp.where(field == per_group, joined >> OWNER_SHIFT, values)
    flat_vmem[...] = jnp.where(field < per_group, joined >> LIVE_BITS, values)
    to_smem = pltpu.make_async_copy(flat_vmem, flat, flat_sem)
    to_smem.start()

    live = jnp.where(field < per_group, joined & ((1 << LIVE_BITS) - 1), 0).astype(F32)
    spread = iota((LANES, LANES), 0) % FIELDS == iota((LANES, LANES), 1) // page_rows
    spread = jnp.where(spread, 1.0, 0.0).astype(BF16)
    chosen = iota((ROUND, LANES), 1) // FIELDS == iota((ROUND, LANES), 0)
    token_row = ((iota((1, LANES), 1) % page_rows) // kv_local).astype(F32)
    picks = [jnp.where(chosen, live[b : b + 1], 0.0) for b in range(steps)]
    wide = nn(jnp.concatenate(picks, axis=0).astype(BF16), spread)
    bias[:, 0, :] = jnp.where(token_row < wide, 0.0, FLOOR)
    to_smem.wait()

    for k in far:
        q_pass_on(k)
    for k in range(chips):
        q_take(k)
    for cp in k_loads:
        cp.wait()

    lane8 = iota((SUB, LANES), 1)
    token = (lane8 % page_rows) // kv_local
    per_head = heads // kv_local
    kv_masks = [lane8 % kv_local == (t * SUB) // per_head for t in range(heads // SUB)]
    blank = jnp.zeros((heads, dim), BF16)

    def by_page(parts):
        got = parts[per_group - 1]
        for i in range(per_group - 2, -1, -1):
            got = jnp.where(lane8 < (i + 1) * page_rows, parts[i], got)
        return got

    def fetch(ref, page_ids):
        return jnp.concatenate([ref[p] for p in page_ids], axis=0)

    def scale_row(ref, page_ids):
        return by_page([jnp.broadcast_to(ref[p], (SUB, LANES)) for p in page_ids])

    def same_owner(it, j):
        return jnp.full((heads, LANES), flat[it, j * FIELDS + per_group + 2], I32) == 0

    def score_step(it, top):
        for pair in range(ROUND // 2):
            js = (2 * pair, 2 * pair + 1)
            ids = [[flat[it, j * FIELDS + i] for i in range(per_group)] for j in js]
            kk = jnp.concatenate([fetch(k_buf, one) for one in ids], axis=1)
            qa, qb = [q_all[flat[it, j * FIELDS + per_group]] for j in js]
            lhs = jnp.concatenate(
                [jnp.concatenate([qa, blank], axis=1), jnp.concatenate([blank, qb], axis=1)], axis=0
            )
            s = nt(lhs, kk)
            for x, j in enumerate(js):
                g = it * ROUND + j
                scale = scale_row(kse, ids[x])
                shift = jnp.broadcast_to(bias[g], (SUB, LANES))
                tiles = []
                for t in range(heads // SUB):
                    tile = s[x * heads + t * SUB : x * heads + (t + 1) * SUB] * scale + shift
                    tiles.append(jnp.where(kv_masks[t], tile, FLOOR))
                tile = jnp.concatenate(tiles, axis=0)
                scores[g] = tile
                mine = jnp.broadcast_to(jnp.max(tile, axis=1, keepdims=True), (heads, LANES))
                top = jnp.where(same_owner(it, j), jnp.maximum(top, mine), mine)
                peaks[g] = top
        return top

    lax.fori_loop(0, steps, score_step, jnp.full((heads, LANES), FLOOR, F32))
    for cp in v_loads:
        cp.wait()

    def value_step(it, carry):
        acc, den = carry
        for pair in range(ROUND // 2):
            js = (2 * pair, 2 * pair + 1)
            ids = [[flat[it, j * FIELDS + i] for i in range(per_group)] for j in js]
            vv = jnp.concatenate([fetch(v_buf, one) for one in ids], axis=1)
            lhs, weights = [], []
            for x, j in enumerate(js):
                weight = jnp.exp(scores[it * ROUND + j] - peaks[flat[it, j * FIELDS + per_group + 1]])
                scale = scale_row(vse, ids[x])
                scaled = [weight[t * SUB : (t + 1) * SUB] * scale for t in range(heads // SUB)]
                lhs.append(jnp.concatenate(scaled, axis=0).astype(BF16))
                weights.append(weight)
            o = nn(jnp.concatenate(lhs, axis=0), vv)
            for x, j in enumerate(js):
                g = it * ROUND + j
                keep = same_owner(it, j)
                mine = o[x * heads : (x + 1) * heads, x * dim : (x + 1) * dim]
                acc = jnp.where(keep, acc + mine, mine)
                den = jnp.where(keep, den + weights[x], weights[x])
                accs[g] = acc
                dens[g] = den
        return acc, den

    zero = jnp.zeros((heads, LANES), F32)
    lax.fori_loop(0, steps, value_step, (zero, zero))

    lane16 = iota((heads, LANES), 1)

    def first_group(dest):
        base = jnp.int32(0)
        for src in range(sources):
            base = base + jnp.where(src < dest, marks[src, rows_here], 0)
        return base

    def local_part(dest, base, r):
        mark = marks[dest, r]
        last = base + (mark >> 1)
        some = (mark & 1).astype(F32)
        den = jnp.broadcast_to(jnp.sum(dens[last], axis=1, keepdims=True), (heads, LANES))
        den = jnp.maximum(den, 0.5)
        num = accs[last] * (some / den)
        return num, (peaks[last] + jnp.log(den)) * some + (some - 1.0) * (-FLOOR)

    def pair_copy(c):
        return remote(pair_send.at[c], pair_recv.at[c], p_send.at[c], p_recv.at[c], req=partner)

    def pair_lse_copy(c):
        return remote(pair_lse_send.at[c], pair_lse_recv.at[c], pl_send.at[c], pl_recv.at[c], req=partner)

    def num_copy(to, owner):
        return remote(
            num_send.at[to], num_recv.at[owner], n_send.at[to], n_recv.at[owner], req=to * 2 + core
        )

    def lse_copy(to, owner):
        return remote(
            lse_send.at[to], lse_recv.at[owner], l_send.at[to], l_recv.at[owner], req=to * 2 + core
        )

    def for_partner(k, carry):
        c = other_chip(chips - 1 - k)
        dest = c * 2 + 1 - core
        base = first_group(dest)
        tile = jnp.full((heads, LANES), FLOOR, F32)
        for r in range(rows_here):
            num, lse = local_part(dest, base, r)
            pair_send[c, r] = num.astype(BF16)
            tile = jnp.where(lane16 == r, lse, tile)
        pair_lse_send[c] = tile
        pair_copy(c).start()
        pair_lse_copy(c).start()
        return carry

    lax.fori_loop(0, chips, for_partner, 0)

    def merge(c, num_at, lse_at):
        dest = c * 2 + core
        base = first_group(dest)
        theirs = pair_lse_recv[c]
        tile = jnp.full((heads, LANES), FLOOR, F32)
        for r in range(rows_here):
            num, lse = local_part(dest, base, r)
            their = jnp.broadcast_to(theirs[:, r : r + 1], (heads, LANES))
            high = jnp.maximum(lse, their)
            a, b = jnp.exp(lse - high), jnp.exp(their - high)
            total = a + b
            got = (num * a + pair_recv[c, r].astype(F32) * b) / total
            num_at[r] = got.astype(BF16)
            tile = jnp.where(lane16 == r, high + jnp.log(total), tile)
        lse_at[...] = tile

    def send_block(k, carry):
        c = other_chip(chips - 1 - k)
        merge(c, num_send.at[c], lse_send.at[c])
        num_copy(c, chip).start()
        lse_copy(c, chip).start()
        return carry

    for k in range(chips - 1, -1, -1):
        pair_lse_copy(other_chip(k)).wait_recv()
        pair_copy(other_chip(k)).wait_recv()
    lax.fori_loop(0, chips - 1, send_block, 0)
    merge(chip, num_recv.at[chip], lse_recv.at[chip])
    for k in far:
        c = other_chip(k)
        lse_copy(c, c).wait_recv()
        num_copy(c, c).wait_recv()

    lses = [lse_recv[s] for s in range(chips)]
    top = functools.reduce(jnp.maximum, lses)
    shares = [jnp.exp(x - top) for x in lses]
    total = functools.reduce(jnp.add, shares)
    shares = [x / total for x in shares]
    for r in range(rows_here):
        got = jnp.zeros((heads, dim), F32)
        for s in range(chips):
            share = jnp.broadcast_to(shares[s][:, r : r + 1], (heads, dim))
            got = got + share * num_recv[s, r].astype(F32)
        mixed[r * heads : (r + 1) * heads, :] = got
    for h in range(heads):
        rows = mixed[pl.ds(h, rows_here, stride=heads), :]
        att_all[me, :, h * dim : (h + 1) * dim] = rows.astype(BF16)

    a_begin, a_pass_on, a_take, a_finish = gather(lambda owner: att_all.at[owner], a_send, a_recv, a_pass)
    a_begin()
    for cp in w_loads:
        cp.wait()

    cols = w_buf.shape[1] // nz
    block_rows = 2 * rows_here

    def term_copy(to, owner, c):
        return remote(
            term_send.at[to, c], term_recv.at[owner, c], z_send.at[to, c], z_recv.at[owner, c], head=to
        )

    def project(picked):
        att = [att_all[pl.ds(2 * c, 2)].reshape(block_rows, width) for c in picked]
        att = jnp.concatenate(att, axis=0)
        spans = [slice(i * block_rows, (i + 1) * block_rows) for i in range(len(picked))]
        if cols % LANES == 0:
            for k in range(1, nz):
                peer = lax.rem(mz + k, nz)
                columns = pl.ds(pl.multiple_of(peer * cols, cols), cols)
                term = nn(att, w_buf[:, columns]).astype(BF16)
                for c, span in zip(picked, spans):
                    term_send[peer, c] = term[span]
                    term_copy(peer, mz, c).start()
            term = nn(att, w_buf[:, pl.ds(pl.multiple_of(mz * cols, cols), cols)])
            for c, span in zip(picked, spans):
                own_terms[c] = term[span]
        else:
            every = nn(att, w_buf[...])
            for c, span in zip(picked, spans):
                for z in range(nz):
                    term_send[z, c] = every[span, z * cols : (z + 1) * cols].astype(BF16)
                for k in range(1, nz):
                    term_copy(lax.rem(mz + k, nz), mz, c).start()
                own_terms[c] = term_send[mz, c].astype(F32)

    order = list(range(1, chips))
    a_take(0)
    project([other_chip(0)])
    for k in order:
        a_pass_on(k)
    for k in order:
        a_take(k)
    project([other_chip(k) for k in order])
    for k in [0] + order:
        c = other_chip(k)
        got = own_terms[c]
        for z in range(1, nz):
            peer = lax.rem(mz + z, nz)
            term_copy(peer, peer, c).wait_recv()
            got = got + term_recv[peer, c].astype(F32)
        out_ref[pl.ds(pl.multiple_of(c * block_rows, block_rows), block_rows), :] = got.astype(BF16)

    for k in range(1, sources):
        peer = lax.rem(me + k, sources)
        info_copy(peer, me).wait_send()
    q_finish()
    a_finish()
    for c in range(chips):
        pair_copy(c).wait_send()
        pair_lse_copy(c).wait_send()
    for k in far:
        c = other_chip(k)
        num_copy(c, chip).wait_send()
        lse_copy(c, chip).wait_send()
    for k in range(1, nz):
        for c in range(chips):
            term_copy(lax.rem(mz + k, nz), mz, c).wait_send()


def on_device(
    queries,
    k_codes,
    value_quantized_codes,
    key_page_scale,
    value_page_scale,
    lengths,
    page_table,
    out_weight,
):
    pages, page_size, kv_local, dim = k_codes.shape
    rows_here, heads, _ = queries.shape
    sources, nz = lax.axis_size("req"), lax.axis_size("head")
    requests = rows_here * sources
    page_rows = page_size * kv_local
    per_group = LANES // page_rows
    group_bound = (pages + (per_group - 1) * requests) // per_group
    n_groups = -(-group_bound // ROUND) * ROUND
    list_bound = (pages + (per_group - 1) * rows_here) // per_group
    list_rows = -(-list_bound // ROUND)
    info_rows = -(-(list_rows + 1) // SUB) * SUB
    flat_rows = -(-(n_groups // ROUND) // SUB) * SUB
    mark_rows = -(-sources // SUB) * SUB
    chips = sources // 2
    k_rows = k_codes.reshape(pages, page_rows, dim)
    v_rows = value_quantized_codes.reshape(pages, page_rows, dim)
    width = heads * dim
    columns = out_weight.shape[1]
    cfg = dict(
        sources=sources,
        nz=nz,
        rows_here=rows_here,
        heads=heads,
        dim=dim,
        pages=pages,
        page_rows=page_rows,
        page_size=page_size,
        n_groups=n_groups,
        per_group=per_group,
        list_rows=list_rows,
    )
    vmem = pl.BlockSpec(memory_space=pltpu.VMEM)
    smem = pl.BlockSpec(memory_space=pltpu.SMEM)
    hbm = pl.BlockSpec(memory_space=pl.ANY)
    dma = pltpu.SemaphoreType.DMA
    info = pl.pallas_call(
        functools.partial(list_kernel, cfg),
        out_shape=jax.ShapeDtypeStruct((sources, info_rows, LANES), I32),
        in_specs=[smem, vmem],
        out_specs=vmem,
        name="lists",
    )(lengths, page_table)
    return pl.pallas_call(
        functools.partial(kernel, cfg),
        out_shape=jax.ShapeDtypeStruct((requests, columns // nz), BF16),
        in_specs=[hbm] * 7,
        out_specs=vmem,
        scratch_shapes=[
            pltpu.VMEM(info.shape, I32),
            pltpu.VMEM((kv_local, pages), F32),
            pltpu.VMEM((kv_local, pages), F32),
            pltpu.VMEM(info.shape, I32),
            pltpu.VMEM((mark_rows, LANES), I32),
            pltpu.SMEM((mark_rows, LANES), I32),
            pltpu.VMEM((flat_rows, LANES), I32),
            pltpu.SMEM((flat_rows, LANES), I32),
            pltpu.VMEM((requests, heads, dim), BF16),
            pltpu.VMEM(k_rows.shape, BF16),
            pltpu.VMEM(v_rows.shape, BF16),
            pltpu.VMEM(out_weight.shape, BF16),
            pltpu.VMEM((pages, 1, LANES), F32),
            pltpu.VMEM((pages, 1, LANES), F32),
            pltpu.VMEM((n_groups, 1, LANES), F32),
            pltpu.VMEM((n_groups, heads, LANES), F32),
            pltpu.VMEM((n_groups, heads, LANES), F32),
            pltpu.VMEM((n_groups, heads, LANES), F32),
            pltpu.VMEM((n_groups, heads, LANES), F32),
            pltpu.VMEM((chips, rows_here, heads, dim), BF16),
            pltpu.VMEM((chips, heads, LANES), F32),
            pltpu.VMEM((chips, rows_here, heads, dim), BF16),
            pltpu.VMEM((chips, heads, LANES), F32),
            pltpu.VMEM((chips, rows_here, heads, dim), BF16),
            pltpu.VMEM((chips, heads, LANES), F32),
            pltpu.VMEM((chips, rows_here, heads, dim), BF16),
            pltpu.VMEM((chips, heads, LANES), F32),
            pltpu.VMEM((rows_here * heads, dim), F32),
            pltpu.VMEM((sources, rows_here, width), BF16),
            pltpu.VMEM((nz, chips, 2 * rows_here, columns // nz), BF16),
            pltpu.VMEM((nz, chips, 2 * rows_here, columns // nz), BF16),
            pltpu.VMEM((chips, 2 * rows_here, columns // nz), F32),
            dma,
            dma((3, 4)),
            dma,
            dma((3,)),
            dma,
            dma,
            dma((sources,)),
            dma((sources,)),
            dma((sources,)),
            dma((sources,)),
            dma((sources,)),
            dma((chips,)),
            dma((chips,)),
            dma((chips,)),
            dma((chips,)),
            dma((chips,)),
            dma((chips,)),
            dma((chips,)),
            dma((chips,)),
            dma((sources,)),
            dma((sources,)),
            dma((sources,)),
            dma((nz, chips)),
            dma((nz, chips)),
        ],
        compiler_params=pltpu.CompilerParams(
            vmem_limit_bytes=62 * 1024 * 1024, collective_id=0, has_side_effects=True
        ),
        name="paged",
    )(
        info,
        key_page_scale.T,
        value_page_scale.T,
        queries,
        k_rows,
        v_rows,
        out_weight,
    )


def solution(mesh):
    in_specs = (
        P("req", "head", None),
        P("req", None, "head", None),
        P("req", None, "head", None),
        P("req", "head"),
        P("req", "head"),
        P("req"),
        P("req", None),
        P("head", "req"),
    )
    out_specs = P(None, ("req", "head"))
    return jax.shard_map(
        on_device, mesh=mesh, in_specs=in_specs, out_specs=out_specs, check_vma=False
    )
```

```python
import functools
import math

import jax
import jax.numpy as jnp
from jax import lax
from jax.experimental import pallas as pl
from jax.experimental.pallas import tpu as pltpu
from jax.sharding import PartitionSpec as P

MESH = pl.DeviceIdType.MESH
FLOOR = -1e30
DROP = -3e38
LANES = 128
SUB = 8
LIVE_BITS = 5
OWNER_SHIFT = 7
FIELDS = 8
ROUND = LANES // FIELDS
F32 = jnp.float32
BF16 = jnp.bfloat16
I32 = jnp.int32


def nt(a, b):
    return lax.dot_general(a, b, (((1,), (1,)), ((), ())), preferred_element_type=F32)


def nn(a, b):
    return jnp.dot(a, b, preferred_element_type=F32)


def iota(shape, axis):
    return lax.broadcasted_iota(I32, shape, axis)


def list_kernel(cfg, lengths_ref, table_ref, out_ref):
    sources, rows_here, pages = cfg["sources"], cfg["rows_here"], cfg["pages"]
    page_size, per_group = cfg["page_size"], cfg["per_group"]
    list_rows = cfg["list_rows"]
    shape = (rows_here, LANES)
    row_id = iota(shape, 0)
    lengths = jnp.zeros(shape, I32)
    for r in range(rows_here):
        lengths = jnp.where(row_id == r, lengths_ref[r], lengths)
    live = jnp.minimum(lengths - iota(shape, 1) * page_size, page_size)
    table = table_ref[...]
    locals_, mines = [], []
    for d in range(sources):
        local = table - d * pages
        locals_.append(local)
        mines.append((live > 0) & (local >= 0) & (local < pages))
    flag = jnp.concatenate([jnp.where(m, 1.0, 0.0) for m in mines], axis=0).astype(BF16)
    total = sources * rows_here
    up = jnp.where(iota((LANES, LANES), 0) < iota((LANES, LANES), 1), 1.0, 0.0).astype(BF16)
    before = nn(flag, up)
    count = nn(flag, jnp.ones((LANES, LANES), BF16))
    need = jnp.floor((count + (per_group - 1)) * (1.0 / per_group))
    i, j = iota((total, total), 0), iota((total, total), 1)
    tri = jnp.where((i >= j) & (i // rows_here == j // rows_here), 1.0, 0.0).astype(BF16)
    ends = nn(tri, need.astype(BF16))
    starts = ends - need
    before, starts_int, need_int = before.astype(I32), starts.astype(I32), need.astype(I32)

    high = jnp.full(shape, -1, I32)
    low, lead, page, rest = high, high, high, high
    for d in range(sources):
        rows = slice(d * rows_here, (d + 1) * rows_here)
        step = before[rows] >> 2
        group = starts_int[rows] + step
        column = (group & (ROUND - 1)) * FIELDS
        place = before[rows] & 3
        high = jnp.where(mines[d], d * list_rows + group // ROUND, high)
        low = jnp.where(mines[d], column + place, low)
        lead = jnp.where(mines[d] & (place == 0), column + per_group, lead)
        page = jnp.where(mines[d], locals_[d], page)
        left = (need_int[rows] - 1 - step) * 2 + jnp.where(step == 0, 1, 0)
        rest = jnp.where(mines[d], left, rest)
    one = (page >> 2).astype(F32)
    two = ((page & 3) * (1 << LIVE_BITS) + live).astype(F32)
    rest = rest.astype(F32)
    hi_rows = -(-(sources * list_rows) // 16) * 16
    hi_iota, lo_iota = iota((hi_rows, LANES), 0), iota((LANES, LANES), 0)
    lefts, rights = [], []
    for r in range(rows_here):
        row = slice(r, r + 1)
        lefts.append(jnp.where(hi_iota == high[row], 1.0, 0.0).astype(BF16))
        same, head = lo_iota == low[row], lo_iota == lead[row]
        pair = [
            jnp.where(same, one[row], jnp.where(head, float(r), 0.0)),
            jnp.where(same, two[row], jnp.where(head, rest[row], 0.0)),
        ]
        rights.append(jnp.concatenate(pair, axis=0).astype(BF16))
    found = nt(jnp.concatenate(lefts, axis=1), jnp.concatenate(rights, axis=1))
    found = (found[:, :LANES] * float(4 << LIVE_BITS) + found[:, LANES:]).astype(I32)

    diag = row_id == iota(shape, 1)
    for d in range(sources):
        rows = slice(d * rows_here, (d + 1) * rows_here)
        end, some = ends[rows], need[rows] > 0.5
        out_ref[d, :list_rows, :] = found[d * list_rows : (d + 1) * list_rows]
        mark = jnp.maximum(end - 1.0, 0.0) * 2.0 + jnp.where(some, 1.0, 0.0)
        mark = jnp.sum(jnp.where(diag, mark, 0.0), axis=0, keepdims=True)
        size = jnp.max(end, axis=0, keepdims=True)
        mark = jnp.where(iota((1, LANES), 1) == rows_here, size, mark)
        out_ref[d, list_rows : list_rows + 1, :] = mark.astype(I32)


def kernel(
    cfg,
    info_hbm,
    kscale_hbm,
    vscale_hbm,
    q_hbm,
    k_hbm,
    v_hbm,
    w_hbm,
    out_ref,
    info_ref,
    kscale_ref,
    vscale_ref,
    info_all,
    mark_vmem,
    marks,
    flat_vmem,
    flat,
    q_all,
    k_buf,
    v_buf,
    w_buf,
    kse,
    vse,
    bias,
    scores,
    peaks,
    dens,
    accs,
    pair_send,
    pair_lse_send,
    pair_recv,
    pair_lse_recv,
    num_send,
    lse_send,
    num_recv,
    lse_recv,
    mixed,
    att_all,
    term_send,
    term_recv,
    own_terms,
    q_sem,
    load_sems,
    info_sem,
    small_sems,
    mark_sem,
    flat_sem,
    t_send,
    t_recv,
    q_send,
    q_recv,
    q_pass,
    p_send,
    p_recv,
    pl_send,
    pl_recv,
    n_send,
    n_recv,
    l_send,
    l_recv,
    a_send,
    a_recv,
    a_pass,
    z_send,
    z_recv,
):
    sources, nz = cfg["sources"], cfg["nz"]
    rows_here, heads, dim = cfg["rows_here"], cfg["heads"], cfg["dim"]
    pages, page_rows, page_size = cfg["pages"], cfg["page_rows"], cfg["page_size"]
    requests = rows_here * sources
    kv_local = page_rows // page_size
    per_group = LANES // page_rows
    n_groups = cfg["n_groups"]
    steps = n_groups // ROUND
    width = heads * dim
    me = lax.axis_index("req")
    mz = lax.axis_index("head")
    chips = sources // 2
    chip, core = me // 2, lax.rem(me, 2)
    partner = me + 1 - 2 * core

    def other_chip(k):
        return lax.rem(chip + k, chips)

    far = range(chips - 1, 0, -1)
    list_rows = cfg["list_rows"]
    flat_rows = flat_vmem.shape[0]

    barrier = pltpu.get_barrier_semaphore()
    for k in range(1, sources):
        pl.semaphore_signal(
            barrier, inc=1, device_id={"req": lax.rem(me + k, sources)}, device_id_type=MESH
        )
    for k in range(1, nz):
        pl.semaphore_signal(barrier, inc=1, device_id={"head": lax.rem(mz + k, nz)}, device_id_type=MESH)
    q_load = pltpu.make_async_copy(q_hbm, q_all.at[pl.ds(me * rows_here, rows_here)], q_sem)
    q_load.start()
    info_load = pltpu.make_async_copy(info_hbm.at[me], info_all.at[me], info_sem)
    info_load.start()
    smalls = []
    pairs = ((info_hbm, info_ref), (kscale_hbm, kscale_ref), (vscale_hbm, vscale_ref))
    for n, (src, dst) in enumerate(pairs):
        cp = pltpu.make_async_copy(src, dst, small_sems.at[n])
        cp.start()
        smalls.append(cp)

    pl.semaphore_wait(barrier, sources + nz - 2)

    def info_copy(peer, owner):
        return pltpu.make_async_remote_copy(
            src_ref=info_ref.at[peer],
            dst_ref=info_all.at[owner],
            send_sem=t_send.at[peer],
            recv_sem=t_recv.at[owner],
            device_id={"req": peer},
            device_id_type=MESH,
        )

    def remote(src, dst, send, recv, **where):
        return pltpu.make_async_remote_copy(
            src_ref=src,
            dst_ref=dst,
            send_sem=send,
            recv_sem=recv,
            device_id=where,
            device_id_type=MESH,
        )

    def gather(rows_of, send, recv, passing):
        def direct(peer, owner):
            return remote(rows_of(owner), rows_of(owner), send.at[peer], recv.at[owner], req=peer)

        def onward(owner):
            return remote(rows_of(owner), rows_of(owner), passing.at[owner], recv.at[owner], req=partner)

        def begin():
            for k in far:
                direct(other_chip(k) * 2 + core, me).start()
            direct(partner, me).start()

        def pass_on(k):
            owner = other_chip(k) * 2 + core
            direct(owner, owner).wait_recv()
            onward(owner).start()

        def take(k):
            owner = other_chip(k) * 2 + 1 - core
            if k == 0:
                direct(partner, partner).wait_recv()
            else:
                onward(owner).wait_recv()

        def finish():
            direct(partner, me).wait_send()
            for k in far:
                owner = other_chip(k) * 2 + core
                direct(owner, me).wait_send()
                onward(owner).wait_send()

        return begin, pass_on, take, finish

    q_begin, q_pass_on, q_take, q_finish = gather(
        lambda owner: q_all.at[pl.ds(owner * rows_here, rows_here)], q_send, q_recv, q_pass
    )
    smalls[0].wait()
    for k in range(sources - 1, 0, -1):
        info_copy(lax.rem(me + k, sources), me).start()
    q_load.wait()
    for cp in smalls[1:]:
        cp.wait()
    q_begin()
    loads = []
    parts = load_sems.shape[1]
    for which, (src, dst) in enumerate(((k_hbm, k_buf), (v_hbm, v_buf), (w_hbm, w_buf))):
        chunk = src.shape[0] // parts
        for c in range(parts):
            rows = pl.ds(c * chunk, chunk)
            cp = pltpu.make_async_copy(src.at[rows], dst.at[rows], load_sems.at[which, c])
            cp.start()
            loads.append(cp)
    k_loads, v_loads, w_loads = loads[:parts], loads[parts : 2 * parts], loads[2 * parts :]

    lane_sub = iota((LANES, LANES), 0)
    for src, dst, factor in ((kscale_ref, kse, 1.0 / math.sqrt(dim)), (vscale_ref, vse, 1.0)):
        for b in range(pages // LANES):
            cols = slice(b * LANES, (b + 1) * LANES)
            both = src[kv_local - 1 : kv_local, cols]
            for v in range(kv_local - 1):
                both = jnp.where(lane_sub % kv_local == v, src[v : v + 1, cols], both)
            both = jnp.broadcast_to(both * factor, (LANES, LANES)).T
            dst[b * LANES : (b + 1) * LANES, 0, :] = both

    info_load.wait()
    for k in range(1, sources):
        peer = lax.rem(me + k, sources)
        info_copy(peer, peer).wait_recv()
    for src in range(sources):
        mark_vmem[src : src + 1, :] = info_all[src, list_rows : list_rows + 1, :]
    to_marks = pltpu.make_async_copy(mark_vmem, marks, mark_sem)
    to_marks.start()
    size_lane = iota((1, LANES), 1) == rows_here

    shape = (flat_rows, LANES)
    lane, field = iota(shape, 1), iota(shape, 1) % FIELDS
    group = iota(shape, 0) * ROUND + lane // FIELDS
    joined = jnp.zeros(shape, I32)
    base = jnp.int32(0)
    for src in range(sources):
        size = jnp.sum(jnp.where(size_lane, info_all[src, list_rows : list_rows + 1, :], 0))
        rows = min(flat_rows, info_all.shape[1])
        one = info_all[src, :rows, :]
        if rows < flat_rows:
            one = jnp.concatenate([one, jnp.zeros((flat_rows - rows, LANES), I32)], axis=0)
        one = jnp.where(field == per_group, one + (src * rows_here << OWNER_SHIFT), one)
        move = (base & (ROUND - 1)) * FIELDS
        one = pltpu.roll(one, move, axis=1)
        one = jnp.where(lane < move, pltpu.roll(one, 1, axis=0), one)
        one = pltpu.roll(one, base // ROUND, axis=0)
        joined = jnp.where((group >= base) & (group < base + size), one, joined)
        base = base + size
    low_bits = (1 << OWNER_SHIFT) - 1
    last = group + ((pltpu.roll(joined, 1, axis=1) & low_bits) >> 1)
    fresh = pltpu.roll(joined, 2, axis=1) & 1
    values = jnp.where(field == per_group + 1, last, fresh)
    values = jnp.where(field == per_group, joined >> OWNER_SHIFT, values)
    flat_vmem[...] = jnp.where(field < per_group, joined >> LIVE_BITS, values)
    to_smem = pltpu.make_async_copy(flat_vmem, flat, flat_sem)
    to_smem.start()

    live = jnp.where(field < per_group, joined & ((1 << LIVE_BITS) - 1), 0).astype(F32)
    spread = iota((LANES, LANES), 0) % FIELDS == iota((LANES, LANES), 1) // page_rows
    spread = jnp.where(spread, 1.0, 0.0).astype(BF16)
    chosen = iota((ROUND, LANES), 1) // FIELDS == iota((ROUND, LANES), 0)
    token_row = ((iota((1, LANES), 1) % page_rows) // kv_local).astype(F32)
    picks = [jnp.where(chosen, live[b : b + 1], 0.0) for b in range(steps)]
    wide = nn(jnp.concatenate(picks, axis=0).astype(BF16), spread)
    bias[:, 0, :] = jnp.where(token_row < wide, 0.0, FLOOR)
    to_smem.wait()
    to_marks.wait()

    for k in far:
        q_pass_on(k)
    for k in range(chips):
        q_take(k)
    for cp in k_loads:
        cp.wait()

    lane8 = iota((SUB, LANES), 1)
    token = (lane8 % page_rows) // kv_local
    per_head = heads // kv_local
    kv_masks = [lane8 % kv_local == (t * SUB) // per_head for t in range(heads // SUB)]
    blank = jnp.zeros((heads, dim), BF16)

    def by_page(parts):
        got = parts[per_group - 1]
        for i in range(per_group - 2, -1, -1):
            got = jnp.where(lane8 < (i + 1) * page_rows, parts[i], got)
        return got

    def fetch(ref, page_ids):
        return jnp.concatenate([ref[p] for p in page_ids], axis=0)

    def scale_row(ref, page_ids):
        return by_page([jnp.broadcast_to(ref[p], (SUB, LANES)) for p in page_ids])

    def same_owner(it, j):
        return jnp.full((heads, LANES), flat[it, j * FIELDS + per_group + 2], I32) == 0

    def peak_of(g):
        return jnp.broadcast_to(jnp.max(peaks[g], axis=1, keepdims=True), (heads, LANES))

    def score_step(it, top):
        for pair in range(ROUND // 2):
            js = (2 * pair, 2 * pair + 1)
            ids = [[flat[it, j * FIELDS + i] for i in range(per_group)] for j in js]
            kk = jnp.concatenate([fetch(k_buf, one) for one in ids], axis=1)
            qa, qb = [q_all[flat[it, j * FIELDS + per_group]] for j in js]
            lhs = jnp.concatenate(
                [jnp.concatenate([qa, blank], axis=1), jnp.concatenate([blank, qb], axis=1)], axis=0
            )
            s = nt(lhs, kk)
            for x, j in enumerate(js):
                g = it * ROUND + j
                scale = scale_row(kse, ids[x])
                shift = jnp.broadcast_to(bias[g], (SUB, LANES))
                tiles = []
                for t in range(heads // SUB):
                    tile = s[x * heads + t * SUB : x * heads + (t + 1) * SUB] * scale + shift
                    tiles.append(jnp.where(kv_masks[t], tile, FLOOR))
                tile = jnp.concatenate(tiles, axis=0)
                scores[g] = tile
                top = jnp.where(same_owner(it, j), jnp.maximum(top, tile), tile)
                peaks[g] = top
        return top

    lax.fori_loop(0, steps, score_step, jnp.full((heads, LANES), FLOOR, F32))
    for cp in v_loads:
        cp.wait()

    def value_step(it, carry):
        acc, den = carry
        for pair in range(ROUND // 2):
            js = (2 * pair, 2 * pair + 1)
            ids = [[flat[it, j * FIELDS + i] for i in range(per_group)] for j in js]
            vv = jnp.concatenate([fetch(v_buf, one) for one in ids], axis=1)
            lhs, weights = [], []
            for x, j in enumerate(js):
                weight = jnp.exp(scores[it * ROUND + j] - peak_of(flat[it, j * FIELDS + per_group + 1]))
                scale = scale_row(vse, ids[x])
                scaled = [weight[t * SUB : (t + 1) * SUB] * scale for t in range(heads // SUB)]
                lhs.append(jnp.concatenate(scaled, axis=0).astype(BF16))
                weights.append(weight)
            o = nn(jnp.concatenate(lhs, axis=0), vv)
            for x, j in enumerate(js):
                g = it * ROUND + j
                keep = same_owner(it, j)
                mine = o[x * heads : (x + 1) * heads, x * dim : (x + 1) * dim]
                acc = jnp.where(keep, acc + mine, mine)
                den = jnp.where(keep, den + weights[x], weights[x])
                accs[g] = acc
                dens[g] = den
        return acc, den

    zero = jnp.zeros((heads, LANES), F32)
    lax.fori_loop(0, steps, value_step, (zero, zero))

    lane16 = iota((heads, LANES), 1)

    def first_group(dest):
        base = jnp.int32(0)
        for src in range(sources):
            base = base + jnp.where(src < dest, marks[src, rows_here], 0)
        return base

    def local_part(dest, base, r):
        mark = marks[dest, r]
        last = base + (mark >> 1)
        some = (mark & 1).astype(F32)
        den = jnp.broadcast_to(jnp.sum(dens[last], axis=1, keepdims=True), (heads, LANES))
        den = jnp.maximum(den, 0.5)
        num = accs[last] * (some / den)
        return num, (peak_of(last) + jnp.log(den)) * some + (some - 1.0) * (-FLOOR)

    def pair_copy(c):
        return remote(pair_send.at[c], pair_recv.at[c], p_send.at[c], p_recv.at[c], req=partner)

    def pair_lse_copy(c):
        return remote(pair_lse_send.at[c], pair_lse_recv.at[c], pl_send.at[c], pl_recv.at[c], req=partner)

    def num_copy(to, owner):
        return remote(
            num_send.at[to], num_recv.at[owner], n_send.at[to], n_recv.at[owner], req=to * 2 + core
        )

    def lse_copy(to, owner):
        return remote(
            lse_send.at[to], lse_recv.at[owner], l_send.at[to], l_recv.at[owner], req=to * 2 + core
        )

    def for_partner(k, carry):
        c = other_chip(chips - 1 - k)
        dest = c * 2 + 1 - core
        base = first_group(dest)
        tile = jnp.full((heads, LANES), FLOOR, F32)
        for r in range(rows_here):
            num, lse = local_part(dest, base, r)
            pair_send[c, r] = num.astype(BF16)
            tile = jnp.where(lane16 == r, lse, tile)
        pair_lse_send[c] = tile
        pair_copy(c).start()
        pair_lse_copy(c).start()
        return carry

    lax.fori_loop(0, chips, for_partner, 0)

    def merge(c, num_at, lse_at):
        dest = c * 2 + core
        base = first_group(dest)
        theirs = pair_lse_recv[c]
        tile = jnp.full((heads, LANES), FLOOR, F32)
        for r in range(rows_here):
            num, lse = local_part(dest, base, r)
            their = jnp.broadcast_to(theirs[:, r : r + 1], (heads, LANES))
            high = jnp.maximum(lse, their)
            a, b = jnp.exp(lse - high), jnp.exp(their - high)
            total = a + b
            got = (num * a + pair_recv[c, r].astype(F32) * b) / total
            num_at[r] = got.astype(BF16)
            tile = jnp.where(lane16 == r, high + jnp.log(total), tile)
        lse_at[...] = tile

    def send_block(k, carry):
        c = other_chip(chips - 1 - k)
        merge(c, num_send.at[c], lse_send.at[c])
        num_copy(c, chip).start()
        lse_copy(c, chip).start()
        return carry

    for k in range(chips - 1, -1, -1):
        pair_lse_copy(other_chip(k)).wait_recv()
        pair_copy(other_chip(k)).wait_recv()
    lax.fori_loop(0, chips - 1, send_block, 0)
    merge(chip, num_recv.at[chip], lse_recv.at[chip])
    for k in far:
        c = other_chip(k)
        lse_copy(c, c).wait_recv()
        num_copy(c, c).wait_recv()

    lses = [lse_recv[s] for s in range(chips)]
    top = functools.reduce(jnp.maximum, lses)
    shares = [jnp.exp(x - top) for x in lses]
    total = functools.reduce(jnp.add, shares)
    shares = [x / total for x in shares]
    for r in range(rows_here):
        got = jnp.zeros((heads, dim), F32)
        for s in range(chips):
            share = jnp.broadcast_to(shares[s][:, r : r + 1], (heads, dim))
            got = got + share * num_recv[s, r].astype(F32)
        mixed[r * heads : (r + 1) * heads, :] = got
    for h in range(heads):
        rows = mixed[pl.ds(h, rows_here, stride=heads), :]
        att_all[me, :, h * dim : (h + 1) * dim] = rows.astype(BF16)

    a_begin, a_pass_on, a_take, a_finish = gather(lambda owner: att_all.at[owner], a_send, a_recv, a_pass)
    a_begin()
    for cp in w_loads:
        cp.wait()

    cols = w_buf.shape[1] // nz
    block_rows = 2 * rows_here

    def term_copy(to, owner, c):
        return remote(
            term_send.at[to, c], term_recv.at[owner, c], z_send.at[to, c], z_recv.at[owner, c], head=to
        )

    def project(picked):
        att = [att_all[pl.ds(2 * c, 2)].reshape(block_rows, width) for c in picked]
        att = jnp.concatenate(att, axis=0)
        spans = [slice(i * block_rows, (i + 1) * block_rows) for i in range(len(picked))]
        if cols % LANES == 0:
            for k in range(1, nz):
                peer = lax.rem(mz + k, nz)
                columns = pl.ds(pl.multiple_of(peer * cols, cols), cols)
                term = nn(att, w_buf[:, columns]).astype(BF16)
                for c, span in zip(picked, spans):
                    term_send[peer, c] = term[span]
                    term_copy(peer, mz, c).start()
            term = nn(att, w_buf[:, pl.ds(pl.multiple_of(mz * cols, cols), cols)])
            for c, span in zip(picked, spans):
                own_terms[c] = term[span]
        else:
            every = nn(att, w_buf[...])
            for c, span in zip(picked, spans):
                for z in range(nz):
                    term_send[z, c] = every[span, z * cols : (z + 1) * cols].astype(BF16)
                for k in range(1, nz):
                    term_copy(lax.rem(mz + k, nz), mz, c).start()
                own_terms[c] = term_send[mz, c].astype(F32)

    order = list(range(1, chips))
    a_take(0)
    project([other_chip(0)])
    for k in order:
        a_pass_on(k)
    for k in order:
        a_take(k)
    project([other_chip(k) for k in order])
    for k in [0] + order:
        c = other_chip(k)
        got = own_terms[c]
        for z in range(1, nz):
            peer = lax.rem(mz + z, nz)
            term_copy(peer, peer, c).wait_recv()
            got = got + term_recv[peer, c].astype(F32)
        out_ref[pl.ds(pl.multiple_of(c * block_rows, block_rows), block_rows), :] = got.astype(BF16)

    for k in range(1, sources):
        peer = lax.rem(me + k, sources)
        info_copy(peer, me).wait_send()
    q_finish()
    a_finish()
    for c in range(chips):
        pair_copy(c).wait_send()
        pair_lse_copy(c).wait_send()
    for k in far:
        c = other_chip(k)
        num_copy(c, chip).wait_send()
        lse_copy(c, chip).wait_send()
    for k in range(1, nz):
        for c in range(chips):
            term_copy(lax.rem(mz + k, nz), mz, c).wait_send()


def on_device(
    queries,
    k_codes,
    value_quantized_codes,
    key_page_scale,
    value_page_scale,
    lengths,
    page_table,
    out_weight,
):
    pages, page_size, kv_local, dim = k_codes.shape
    rows_here, heads, _ = queries.shape
    sources, nz = lax.axis_size("req"), lax.axis_size("head")
    requests = rows_here * sources
    page_rows = page_size * kv_local
    per_group = LANES // page_rows
    group_bound = (pages + (per_group - 1) * requests) // per_group
    n_groups = -(-group_bound // ROUND) * ROUND
    list_bound = (pages + (per_group - 1) * rows_here) // per_group
    list_rows = -(-list_bound // ROUND)
    info_rows = -(-(list_rows + 1) // SUB) * SUB
    flat_rows = -(-(n_groups // ROUND) // SUB) * SUB
    mark_rows = -(-sources // SUB) * SUB
    chips = sources // 2
    k_rows = k_codes.reshape(pages, page_rows, dim)
    v_rows = value_quantized_codes.reshape(pages, page_rows, dim)
    width = heads * dim
    columns = out_weight.shape[1]
    cfg = dict(
        sources=sources,
        nz=nz,
        rows_here=rows_here,
        heads=heads,
        dim=dim,
        pages=pages,
        page_rows=page_rows,
        page_size=page_size,
        n_groups=n_groups,
        per_group=per_group,
        list_rows=list_rows,
    )
    vmem = pl.BlockSpec(memory_space=pltpu.VMEM)
    smem = pl.BlockSpec(memory_space=pltpu.SMEM)
    hbm = pl.BlockSpec(memory_space=pl.ANY)
    dma = pltpu.SemaphoreType.DMA
    info = pl.pallas_call(
        functools.partial(list_kernel, cfg),
        out_shape=jax.ShapeDtypeStruct((sources, info_rows, LANES), I32),
        in_specs=[smem, vmem],
        out_specs=vmem,
        name="lists",
    )(lengths, page_table)
    return pl.pallas_call(
        functools.partial(kernel, cfg),
        out_shape=jax.ShapeDtypeStruct((requests, columns // nz), BF16),
        in_specs=[hbm] * 7,
        out_specs=vmem,
        scratch_shapes=[
            pltpu.VMEM(info.shape, I32),
            pltpu.VMEM((kv_local, pages), F32),
            pltpu.VMEM((kv_local, pages), F32),
            pltpu.VMEM(info.shape, I32),
            pltpu.VMEM((mark_rows, LANES), I32),
            pltpu.SMEM((mark_rows, LANES), I32),
            pltpu.VMEM((flat_rows, LANES), I32),
            pltpu.SMEM((flat_rows, LANES), I32),
            pltpu.VMEM((requests, heads, dim), BF16),
            pltpu.VMEM(k_rows.shape, BF16),
            pltpu.VMEM(v_rows.shape, BF16),
            pltpu.VMEM(out_weight.shape, BF16),
            pltpu.VMEM((pages, 1, LANES), F32),
            pltpu.VMEM((pages, 1, LANES), F32),
            pltpu.VMEM((n_groups, 1, LANES), F32),
            pltpu.VMEM((n_groups, heads, LANES), F32),
            pltpu.VMEM((n_groups, heads, LANES), F32),
            pltpu.VMEM((n_groups, heads, LANES), F32),
            pltpu.VMEM((n_groups, heads, LANES), F32),
            pltpu.VMEM((chips, rows_here, heads, dim), BF16),
            pltpu.VMEM((chips, heads, LANES), F32),
            pltpu.VMEM((chips, rows_here, heads, dim), BF16),
            pltpu.VMEM((chips, heads, LANES), F32),
            pltpu.VMEM((chips, rows_here, heads, dim), BF16),
            pltpu.VMEM((chips, heads, LANES), F32),
            pltpu.VMEM((chips, rows_here, heads, dim), BF16),
            pltpu.VMEM((chips, heads, LANES), F32),
            pltpu.VMEM((rows_here * heads, dim), F32),
            pltpu.VMEM((sources, rows_here, width), BF16),
            pltpu.VMEM((nz, chips, 2 * rows_here, columns // nz), BF16),
            pltpu.VMEM((nz, chips, 2 * rows_here, columns // nz), BF16),
            pltpu.VMEM((chips, 2 * rows_here, columns // nz), F32),
            dma,
            dma((3, 4)),
            dma,
            dma((3,)),
            dma,
            dma,
            dma((sources,)),
            dma((sources,)),
            dma((sources,)),
            dma((sources,)),
            dma((sources,)),
            dma((chips,)),
            dma((chips,)),
            dma((chips,)),
            dma((chips,)),
            dma((chips,)),
            dma((chips,)),
            dma((chips,)),
            dma((chips,)),
            dma((sources,)),
            dma((sources,)),
            dma((sources,)),
            dma((nz, chips)),
            dma((nz, chips)),
        ],
        compiler_params=pltpu.CompilerParams(
            vmem_limit_bytes=62 * 1024 * 1024, collective_id=0, has_side_effects=True
        ),
        name="paged",
    )(
        info,
        key_page_scale.T,
        value_page_scale.T,
        queries,
        k_rows,
        v_rows,
        out_weight,
    )


def solution(mesh):
    in_specs = (
        P("req", "head", None),
        P("req", None, "head", None),
        P("req", None, "head", None),
        P("req", "head"),
        P("req", "head"),
        P("req"),
        P("req", None),
        P("head", "req"),
    )
    out_specs = P(None, ("req", "head"))
    return jax.shard_map(
        on_device, mesh=mesh, in_specs=in_specs, out_specs=out_specs, check_vma=False
    )
```
